128 devices in a mesh: head: 8 (over x, core), ctx: 16 (over z, y).
Axes of the slice: x: 4, y: 4, z: 4, core: 2. Of those that a mesh axis runs over, the one named last changes fastest.
Arguments:
- query_rows: bfloat16 [16384, 4096], P(('head', 'ctx')), may hold values from -6 to 6
- key_rows: bfloat16 [16384, 4096], P(('head', 'ctx')), may hold values from -6 to 6
- value_rows: bfloat16 [16384, 4096], P(('head', 'ctx')), may hold values from -6 to 6
- token_rates: float32 [16384, 16], P(('head', 'ctx')), may hold values from 0.05 to 0.5
- fast_weights: float32 [16, 3, 1024, 256], P('head'), may hold values from -0.4 to 0.4
- momentum: float32 [16, 3, 1024, 256], P('head'), may hold values from -0.12 to 0.12
- out_weight: bfloat16 [4096, 4096], P('head'), may hold values from -0.09375 to 0.09375
Outputs:
- output: bfloat16 [16384, 4096], P(('head', 'ctx'))
The draws below stay inside these ranges and needn't reach their ends.
All inputs are finite; a program needn't handle non-finite values.
Results may differ from the reference program's by a relative error of at most 0.035.
Values may be sent and summed in bfloat16 or wider, within the bound.
A program may use at most 128 MiB of HBM per device.

```python
import math
import jax
import jax.numpy as jnp
from jax import lax

HEADS = 16
D_H = 256
FF = 1024
D = 4096
TOKENS = 16384
N_HEAD = 8


def levels(rng, shape, shards, smallest, high):
    loudness, own = 1.0, jax.random.fold_in(rng, 6)
    for position, shards_of in shards:
        heights = jnp.exp(jax.random.uniform(jax.random.fold_in(own, position), (shards_of,), jnp.float32, smallest / len(shards), high / len(shards)))
        loudness = loudness * jnp.repeat(heights, shape[position] // shards_of).reshape([-1 if axis == position else 1 for axis in range(len(shape))])
    return loudness


def noise(stream_key, shape, width, bound, split=(), held_as=jnp.bfloat16):
    drawn = jax.random.normal(stream_key, shape, jnp.float32) * width
    if len(split) > 0:
        drawn = levels(stream_key, shape, split, -0.22, 0.18) * drawn
    return jnp.clip(drawn, min=-bound, max=bound).astype(held_as)


def setup_inputs(seed: int = 0) -> dict:
    streams_of = jax.random.split(jax.random.key(seed), 8)
    return {
        "query_rows": noise(streams_of[0], (TOKENS, D), 1.0, 6.0, ((0, 128),)),
        "key_rows": noise(streams_of[1], (TOKENS, D), 1.0, 6.0, ((0, 128),)),
        "value_rows": noise(streams_of[2], (TOKENS, D), 1.0, 6.0, ((0, 128),)),
        "token_rates": jnp.clip(jnp.exp(math.log(0.5) - 2.3025851 * jax.random.uniform(streams_of[3], (TOKENS, HEADS), jnp.float32) ** levels(streams_of[3], (TOKENS, HEADS), ((0, 128),), -0.2, 0.2)), 0.05, 0.5),
        "fast_weights": noise(streams_of[4], (HEADS, 3, FF, D_H), 0.0625, 0.4, ((0, 8),), jnp.float32),
        "momentum": noise(streams_of[5], (HEADS, 3, FF, D_H), 0.02, 0.12, ((0, 8),), jnp.float32),
        "out_weight": noise(streams_of[6], (D, D), D ** -0.5, 0.09375, ((0, 8),)),
    }


def head_gradient(key_head, value_head, rate_col, weight_bf, rate_scale):
    pre_act = jnp.dot(key_head, weight_bf[0].T, preferred_element_type=jnp.float32)
    gate_act = jnp.dot(key_head, weight_bf[1].T, preferred_element_type=jnp.float32)
    sigmoid_pre = jax.nn.sigmoid(pre_act)
    silu_pre = pre_act * sigmoid_pre
    hidden = (silu_pre * gate_act).astype(jnp.bfloat16)
    grad_out = (-(rate_col * rate_scale) * value_head.astype(jnp.float32)).astype(jnp.bfloat16)
    grad_hidden = jnp.dot(grad_out, weight_bf[2].T, preferred_element_type=jnp.float32)
    grad_pre = (grad_hidden * gate_act * (sigmoid_pre * (1.0 + pre_act * (1.0 - sigmoid_pre)))).astype(jnp.bfloat16)
    grad_gate = (grad_hidden * silu_pre).astype(jnp.bfloat16)
    return jnp.stack([jnp.dot(grad_pre.T, key_head, preferred_element_type=jnp.float32), jnp.dot(grad_gate.T, key_head, preferred_element_type=jnp.float32), jnp.dot(hidden.T, grad_out, preferred_element_type=jnp.float32)])

def rescale(updated, previous_rows, previous_full, column_new):
    row_old = jnp.sqrt(lax.optimization_barrier(jnp.sum(jnp.square(previous_rows[:, :2]), axis=3, keepdims=True)))
    row_new = lax.optimization_barrier(jnp.sum(jnp.square(updated[:, :2]), axis=3, keepdims=True))
    first = updated[:, :2] * row_old / jnp.sqrt(row_new + 1e-06)
    column_old = jnp.sqrt(lax.optimization_barrier(jnp.sum(jnp.square(previous_full[:, 2]), axis=1, keepdims=True)))
    second = updated[:, 2] * column_old / jnp.sqrt(column_new + 1e-06)
    return jnp.concatenate([first, second[:, None]], axis=1)

def apply_head(query_head, normed_head):
    pre_act = jnp.dot(query_head, normed_head[0].T, preferred_element_type=jnp.float32)
    gate_act = jnp.dot(query_head, normed_head[1].T, preferred_element_type=jnp.float32)
    hidden = (pre_act * jax.nn.sigmoid(pre_act) * gate_act).astype(jnp.bfloat16)
    return jnp.dot(hidden, normed_head[2], preferred_element_type=jnp.float32).astype(jnp.bfloat16)

def reference(query_rows, key_rows, value_rows, token_rates, fast_weights, momentum, out_weight):
    rate_scale = float(TOKENS) ** (-0.5)
    gradient_list = []
    for head_index in range(HEADS):
        lower = head_index * D_H
        weight_bf = fast_weights[head_index].astype(jnp.bfloat16)
        gradient_list.append(head_gradient(key_rows[:, lower:lower + D_H], value_rows[:, lower:lower + D_H], token_rates[:, head_index:head_index + 1], weight_bf, rate_scale))
    gradients = jnp.stack(gradient_list)
    updated = fast_weights - (0.9 * momentum + gradients)
    column_new = lax.optimization_barrier(jnp.sum(jnp.square(updated[:, 2]), axis=1, keepdims=True))
    normed = rescale(updated, fast_weights, fast_weights, column_new).astype(jnp.bfloat16)
    mixed_list = []
    for head_index in range(HEADS):
        lower = head_index * D_H
        mixed_list.append(apply_head(query_rows[:, lower:lower + D_H], normed[head_index]))
    mixed = jnp.concatenate(mixed_list, axis=1)
    group_width = D // N_HEAD
    accumulated = jnp.zeros((TOKENS, D), jnp.float32)
    for group_index in range(N_HEAD):
        lower = group_index * group_width
        partial_sum = jnp.dot(mixed[:, lower:lower + group_width], out_weight[lower:lower + group_width], preferred_element_type=jnp.float32).astype(jnp.bfloat16)
        partial_sum = lax.optimization_barrier(partial_sum)
        accumulated = accumulated + partial_sum.astype(jnp.float32)
    return accumulated.astype(jnp.bfloat16)
```

```python
import functools

import jax
import jax.numpy as jnp
from jax import lax
from jax.experimental import pallas as pl
from jax.experimental.pallas import tpu as pltpu
from jax.sharding import PartitionSpec as P

MESH = pl.DeviceIdType.MESH
F32 = jnp.float32
BF16 = jnp.bfloat16

OFFSETS = (
    (0, 0), (0, 1), (0, 3), (0, 2),
    (1, 0), (1, 1), (1, 3), (1, 2),
    (3, 0), (3, 1), (3, 3), (3, 2),
    (2, 0), (2, 1), (2, 3), (2, 2),
)
SEND_ORDER = (1, 4, 8, 2, 12, 3, 5, 9, 6, 10, 13, 14, 7, 11, 15)
NT = (((1,), (1,)), ((), ()))


def dot_nt(a, b):
    return lax.dot_general(a, b, NT, preferred_element_type=F32)


def dot_nn(a, b):
    return jnp.dot(a, b, preferred_element_type=F32)


def kernel(
    rate_scale,
    q_ref, k_ref, v_ref, rates_ref, fast_ref, mom_ref, wout_ref,
    out_ref,
    gsrc, kbuf, gbuf, qbuf, wf, wb, mom, grad,
    csend, crecv, zsend, zrecv, normed, cscale,
    osend, obuf, wout, stash, total, msend, mrecv,
    a2a_send, a2a_recv, loc_sem, w_send, w_recv, cs_sem, cr_sem, zs_sem, zr_sem,
    ns_sem, nr_sem, ps_sem, pr_sem, os_sem, or_sem, ms_sem, mr_sem, wo_send, wo_recv,
):
    head, ctx = lax.axis_index("head"), lax.axis_index("ctx")
    x, c = head // 2, head % 2
    z, y = ctx // 4, ctx % 4
    owner = y // 2
    local = y % 2

    def dev(dx=0, dy=0, dz=0, dc=0):
        return (((x + dx) % 4) * 2 + (c + dc) % 2, ((z + dz) % 4) * 4 + (y + dy) % 4)

    def remote(src, dst, ssem, rsem, where):
        return pltpu.make_async_remote_copy(
            src_ref=src, dst_ref=dst, send_sem=ssem, recv_sem=rsem, device_id=where, device_id_type=MESH
        )

    barrier = pltpu.get_barrier_semaphore()
    for dx, dy in OFFSETS[1:]:
        pl.semaphore_signal(barrier, inc=1, device_id=dev(dx, dy), device_id_type=MESH)
    for dz in (1, 2, 3):
        pl.semaphore_signal(barrier, inc=1, device_id=dev(dz=dz), device_id_type=MESH)
    pl.semaphore_signal(barrier, inc=1, device_id=dev(dc=1), device_id_type=MESH)

    for h in range(16):
        cols = pl.ds(h * 256, 256)
        gsrc[:, cols] = (-(rates_ref[:, h : h + 1] * rate_scale) * v_ref[:, cols].astype(F32)).astype(BF16)

    mine = pl.multiple_of((x * 4 + y) * 256, 256)
    k_own = pltpu.make_async_copy(k_ref.at[:, pl.ds(mine, 256)], kbuf.at[pl.ds(0, 128)], a2a_recv.at[0, 0])
    q_own = pltpu.make_async_copy(q_ref.at[:, pl.ds(mine, 256)], qbuf.at[pl.ds(0, 128)], a2a_recv.at[2, 0])
    k_own.start()
    gbuf[pl.ds(0, 128), :] = gsrc[:, pl.ds(mine, 256)]

    pl.semaphore_wait(barrier, 19)

    def block_copy(kind, source, target, slot):
        dx, dy = OFFSETS[slot]
        to = pl.multiple_of((((x + dx) % 4) * 4 + (y + dy) % 4) * 256, 256)
        return remote(
            source.at[:, pl.ds(to, 256)], target.at[pl.ds(slot * 128, 128)],
            a2a_send.at[kind, slot], a2a_recv.at[kind, slot], dev(dx, dy),
        )

    def weights_in(m):
        return pltpu.make_async_copy(fast_ref.at[local, m], wf.at[m], loc_sem.at[m])

    def weights_over(m):
        return remote(fast_ref.at[local, m], wf.at[m], w_send.at[m], w_recv.at[m], dev(dc=1))

    row_own = pl.multiple_of(c * 512 + z * 128, 128)
    row_other = pl.multiple_of((1 - c) * 512 + z * 128, 128)
    mom_in = pltpu.make_async_copy(mom_ref.at[local, :, pl.ds(row_own, 128)], mom, loc_sem.at[3])
    mom_over = remote(mom_ref.at[local, :, pl.ds(row_other, 128)], mom, w_send.at[3], w_recv.at[3], dev(dc=1))

    a2a = []
    for slot in SEND_ORDER[:3]:
        for kind, source, target in ((0, k_ref, kbuf), (1, gsrc, gbuf)):
            copy = block_copy(kind, source, target, slot)
            copy.start()
            a2a.append(copy)

    @pl.when(c == owner)
    def _():
        for m in range(3):
            weights_over(m).start()
            weights_in(m).start()
        mom_over.start()
        mom_in.start()

    for slot in SEND_ORDER[3:]:
        for kind, source, target in ((0, k_ref, kbuf), (1, gsrc, gbuf)):
            copy = block_copy(kind, source, target, slot)
            copy.start()
            a2a.append(copy)
    for slot in SEND_ORDER:
        copy = block_copy(2, q_ref, qbuf, slot)
        copy.start()
        a2a.append(copy)
    q_own.start()

    for m in range(3):
        @pl.when(c == owner)
        def _():
            weights_in(m).wait()

        @pl.when(c != owner)
        def _():
            weights_over(m).wait_recv()

        wb[m] = wf[m].astype(BF16)

    chunk = 512

    def grad_block(t, first):
        toks = pl.ds(pl.multiple_of(t * 256, 256), 256)

        def body(i, carry):
            rows = pl.ds(pl.multiple_of(i * chunk, chunk), chunk)
            keys, gout = kbuf[toks, :], gbuf[toks, :]
            pre = dot_nt(wb[0, rows, :], keys)
            gate = dot_nt(wb[1, rows, :], keys)
            back = dot_nt(wb[2, rows, :], gout)
            sg = 0.5 + 0.5 * jnp.tanh(0.5 * pre)
            silu = pre * sg
            hidden = (silu * gate).astype(BF16)
            grad_gate = (back * silu).astype(BF16)
            grad_pre = ((back * gate) * (sg + silu - silu * sg)).astype(BF16)
            g0 = dot_nn(grad_pre, keys)
            g1 = dot_nn(grad_gate, keys)
            g2 = dot_nn(hidden, gout)
            if first:
                grad[0, rows, :] = g0
                grad[1, rows, :] = g1
                grad[2, rows, :] = g2
            else:
                grad[0, rows, :] += g0
                grad[1, rows, :] += g1
                grad[2, rows, :] += g2
            return carry

        lax.fori_loop(0, 1024 // chunk, body, 0)

    def slot_wait(kind, target, slot):
        remote(
            target.at[pl.ds(0, 128)], target.at[pl.ds(slot * 128, 128)],
            a2a_send.at[kind, slot], a2a_recv.at[kind, slot], dev(1),
        ).wait_recv()

    k_own.wait()
    slot_wait(0, kbuf, 1)
    slot_wait(1, gbuf, 1)
    grad_block(0, True)

    def later(t, carry):
        for j in range(2):
            slot = 2 * t + j
            slot_wait(0, kbuf, slot)
            slot_wait(1, gbuf, slot)
        grad_block(t, False)
        return carry

    lax.fori_loop(1, 8, later, 0)

    wo_rows = pl.ds(pl.multiple_of(c * 512, 512), 512)
    wo_in = pltpu.make_async_copy(wout_ref, wout.at[wo_rows], loc_sem.at[4])
    wo_over = remote(wout_ref, wout.at[wo_rows], wo_send, wo_recv, dev(dc=1))

    core_copies = []
    for n, dz in enumerate((2, 1, 3, 0)):
        rows = pl.ds(pl.multiple_of((1 - c) * 512 + ((z + dz) % 4) * 128, 128), 128)
        csend[n] = grad[:, rows, :].astype(BF16)
        copy = remote(csend.at[n], crecv.at[n], cs_sem.at[n], cr_sem.at[n], dev(dc=1))
        copy.start()
        core_copies.append(copy)
    z_copies = []
    for n, dz in enumerate((2, 1, 3)):
        rows = pl.ds(pl.multiple_of(c * 512 + ((z + dz) % 4) * 128, 128), 128)
        core_copies[n].wait_recv()
        zsend[n] = (grad[:, rows, :] + crecv[n].astype(F32)).astype(BF16)
        copy = remote(zsend.at[n], zrecv.at[n], zs_sem.at[n], zr_sem.at[n], dev(dz=dz))
        copy.start()
        z_copies.append(copy)
    wo_in.start()
    wo_over.start()
    core_copies[3].wait_recv()
    own = pl.ds(row_own, 128)

    @pl.when(c == owner)
    def _():
        mom_in.wait()

    @pl.when(c != owner)
    def _():
        mom_over.wait_recv()

    base = wf[:, own, :] - 0.9 * mom[...] - (grad[:, own, :] + crecv[3].astype(F32))
    grad[:, own, :] = base
    row_old = jnp.sqrt(jnp.sum(jnp.square(wf[0:2, own, :]), axis=2, keepdims=True))
    column_old = jnp.sqrt(jnp.sum(jnp.square(wf[2]), axis=0, keepdims=True))
    for n in range(3):
        z_copies[n].wait_recv()
    updated = grad[:, own, :] - (zrecv[0].astype(F32) + zrecv[1].astype(F32) + zrecv[2].astype(F32))
    row_new = jnp.sum(jnp.square(updated[0:2]), axis=2, keepdims=True)
    normed[0:2, own, :] = (updated[0:2] * row_old / jnp.sqrt(row_new + 1e-06)).astype(BF16)
    normed[2, own, :] = updated[2].astype(BF16)

    n_copies, p_copies = [], []
    for n, dz in enumerate((2, 1, 3)):
        copy = remote(normed.at[:, own], normed.at[:, own], ns_sem.at[n], nr_sem.at[n], dev(dz=dz))
        copy.start()
        n_copies.append(copy)
    copy = remote(normed.at[:, own], normed.at[:, own], ps_sem.at[3], pr_sem.at[3], dev(dc=1))
    copy.start()
    p_copies.append(copy)
    for n, dz in ((1, 1), (2, 3), (0, 2)):
        n_copies[n].wait_recv()
        rows = pl.ds(pl.multiple_of(c * 512 + ((z - dz) % 4) * 128, 128), 128)
        copy = remote(normed.at[:, rows], normed.at[:, rows], ps_sem.at[n], pr_sem.at[n], dev(dc=1))
        copy.start()
        p_copies.append(copy)
    for copy in p_copies:
        copy.wait_recv()
    column_new = jnp.sum(jnp.square(normed[2].astype(F32)), axis=0, keepdims=True)
    cscale[...] = column_old / jnp.sqrt(column_new + 1e-06)

    q_own.wait()

    def apply_slots(t):
        toks = pl.ds(t * 256, 256)

        def body(i, acc):
            rows = pl.ds(pl.multiple_of(i * chunk, chunk), chunk)
            query = qbuf[toks, :]
            pre = dot_nt(query, normed[0, rows, :])
            gate = dot_nt(query, normed[1, rows, :])
            hidden = (pre * (0.5 + 0.5 * jnp.tanh(0.5 * pre)) * gate).astype(BF16)
            return acc + dot_nn(hidden, normed[2, rows, :])

        acc = lax.fori_loop(0, 1024 // chunk, body, jnp.zeros((256, 256), F32))
        osend[toks, :] = (acc * cscale[...]).astype(BF16)

    my_cols = pl.ds(pl.multiple_of(y * 256, 256), 256)
    o_copies = []
    for t in (6, 7, 4, 5, 2, 3, 0, 1):
        for slot in (2 * t, 2 * t + 1):
            if slot > 0:
                slot_wait(2, qbuf, slot)
        apply_slots(t)
        for slot in (2 * t, 2 * t + 1):
            dx, dy = OFFSETS[slot]
            if dy == 0:
                obuf[pl.ds(dx * 128, 128), my_cols] = osend[pl.ds(slot * 128, 128), :]
            else:
                copy = remote(
                    osend.at[pl.ds(slot * 128, 128)], obuf.at[pl.ds(dx * 128, 128), my_cols],
                    os_sem.at[dx, dy], or_sem.at[dx, dy], dev(dy=-dy),
                )
                copy.start()
                o_copies.append(copy)

    wo_in.wait()
    wo_over.wait_recv()

    def o_wait(dx):
        for dy in (1, 2, 3):
            remote(
                osend.at[pl.ds(0, 128)], obuf.at[pl.ds(dx * 128, 128), pl.ds(0, 256)],
                os_sem.at[dx, dy], or_sem.at[dx, dy], dev(1),
            ).wait_recv()

    def message(kind, j, up):
        return remote(
            msend.at[kind, j], mrecv.at[kind, j], ms_sem.at[kind, j], mr_sem.at[kind, j], dev(1 if up else -1)
        )

    def product(first, rows, j):
        return dot_nn(obuf[pl.ds(first, rows), :], wout[:, pl.ds(pl.multiple_of(j * 512, 512), 512)])

    o_wait(2)

    def far(j, carry):
        msend[0, j] = product(256, 128, j).astype(BF16)
        message(0, j, True).start()
        msend[1, j] = product(256, 128, j + 4).astype(BF16)
        message(1, j, False).start()
        return carry

    lax.fori_loop(0, 4, far, 0)
    o_wait(1)
    o_wait(3)

    def near(j, carry):
        msend[2, j] = product(384, 128, j + 4).astype(BF16)
        message(2, j, True).start()
        msend[3, j] = product(128, 128, j).astype(BF16)
        message(3, j, False).start()
        return carry

    lax.fori_loop(0, 4, near, 0)

    def relay_part(j, carry):
        stash[0, j] = product(384, 128, j)
        stash[1, j] = product(128, 128, j + 4)
        return carry

    lax.fori_loop(0, 4, relay_part, 0)

    def relay(j, carry):
        message(0, j, True).wait_recv()
        msend[4, j] = (stash[0, j] + mrecv[0, j].astype(F32)).astype(BF16)
        message(4, j, True).start()
        message(1, j, False).wait_recv()
        msend[5, j] = (stash[1, j] + mrecv[1, j].astype(F32)).astype(BF16)
        message(5, j, False).start()
        return carry

    lax.fori_loop(0, 4, relay, 0)
    o_wait(0)

    def rest(j, carry):
        total[j] = product(0, 128, j)
        return carry

    lax.fori_loop(0, 8, rest, 0)

    def finish(j, carry):
        low = pl.ds(pl.multiple_of(j * 512, 512), 512)
        high = pl.ds(pl.multiple_of(j * 512 + 2048, 512), 512)
        message(3, j, False).wait_recv()
        message(2, j, True).wait_recv()
        message(4, j, True).wait_recv()
        out_ref[:, low] = (total[j] + mrecv[3, j].astype(F32) + mrecv[4, j].astype(F32)).astype(BF16)
        message(5, j, False).wait_recv()
        out_ref[:, high] = (total[j + 4] + mrecv[2, j].astype(F32) + mrecv[5, j].astype(F32)).astype(BF16)
        return carry

    lax.fori_loop(0, 4, finish, 0)

    for copy in a2a + core_copies + z_copies + n_copies + p_copies + o_copies:
        copy.wait_send()
    wo_over.wait_send()

    @pl.when(c == owner)
    def _():
        for m in range(3):
            weights_over(m).wait_send()
        mom_over.wait_send()

    def drain(j, carry):
        for kind in range(6):
            message(kind, j, kind % 2 == 0).wait_send()
        return carry

    lax.fori_loop(0, 4, drain, 0)


def shards(query_rows, key_rows, value_rows, token_rates, fast_weights, momentum, out_weight):
    tokens = key_rows.shape[0] * lax.axis_size("head") * lax.axis_size("ctx")
    anywhere = pl.BlockSpec(memory_space=pl.ANY)
    vmem = pl.BlockSpec(memory_space=pltpu.VMEM)
    dma = pltpu.SemaphoreType.DMA
    return pl.pallas_call(
        functools.partial(kernel, float(tokens) ** (-0.5)),
        out_shape=jax.ShapeDtypeStruct((128, 4096), BF16),
        in_specs=[anywhere, anywhere, vmem, vmem, anywhere, anywhere, anywhere],
        out_specs=vmem,
        scratch_shapes=[
            pltpu.VMEM((128, 4096), BF16),
            pltpu.VMEM((2048, 256), BF16),
            pltpu.VMEM((2048, 256), BF16),
            pltpu.VMEM((2048, 256), BF16),
            pltpu.VMEM((3, 1024, 256), F32),
            pltpu.VMEM((3, 1024, 256), BF16),
            pltpu.VMEM((3, 128, 256), F32),
            pltpu.VMEM((3, 1024, 256), F32),
            pltpu.VMEM((4, 3, 128, 256), BF16),
            pltpu.VMEM((4, 3, 128, 256), BF16),
            pltpu.VMEM((3, 3, 128, 256), BF16),
            pltpu.VMEM((3, 3, 128, 256), BF16),
            pltpu.VMEM((3, 1024, 256), BF16),
            pltpu.VMEM((1, 256), F32),
            pltpu.VMEM((2048, 256), BF16),
            pltpu.VMEM((512, 1024), BF16),
            pltpu.VMEM((1024, 4096), BF16),
            pltpu.VMEM((2, 4, 128, 512), F32),
            pltpu.VMEM((8, 128, 512), F32),
            pltpu.VMEM((6, 4, 128, 512), BF16),
            pltpu.VMEM((6, 4, 128, 512), BF16),
            dma((3, 16)), dma((3, 16)), dma((5,)), dma((4,)), dma((4,)), dma((4,)), dma((4,)), dma((3,)), dma((3,)),
            dma((3,)), dma((3,)), dma((4,)), dma((4,)), dma((4, 4)), dma((4, 4)), dma((6, 4)), dma((6, 4)), dma(()), dma(()),
        ],
        compiler_params=pltpu.CompilerParams(collective_id=0, has_side_effects=True, vmem_limit_bytes=62 * 2**20),
        name="ttt_layer",
    )(query_rows, key_rows, value_rows, token_rates, fast_weights, momentum, out_weight)


def solution(mesh):
    placed = (
        P(("head", "ctx"), None),
        P(("head", "ctx"), None),
        P(("head", "ctx"), None),
        P(("head", "ctx"), None),
        P("head", None, None, None),
        P("head", None, None, None),
        P("head", None),
    )
    return jax.shard_map(
        shards, mesh=mesh, in_specs=placed, out_specs=P(("head", "ctx"), None), check_vma=False
    )
```

```python
import functools

import jax
import jax.numpy as jnp
from jax import lax
from jax.experimental import pallas as pl
from jax.experimental.pallas import tpu as pltpu
from jax.sharding import PartitionSpec as P

MESH = pl.DeviceIdType.MESH
F32 = jnp.float32
BF16 = jnp.bfloat16

K_OFFSETS = (
    (0, 0), (2, 2), (1, 1), (3, 3),
    (2, 1), (1, 2), (2, 3), (3, 2),
    (2, 0), (0, 2), (1, 3), (3, 1),
    (1, 0), (0, 1), (3, 0), (0, 3),
)
Q_OFFSETS = (
    (0, 0), (0, 1), (0, 3), (0, 2),
    (2, 0), (2, 1), (2, 3), (2, 2),
    (1, 2), (3, 2), (1, 1), (3, 3),
    (1, 3), (3, 1), (1, 0), (3, 0),
)
Q_ORDER = (7, 10, 11, 5, 8, 6, 9, 4, 3, 12, 13, 14, 1, 15, 2)


NT = (((1,), (1,)), ((), ()))


def dot_nt(a, b):
    return lax.dot_general(a, b, NT, preferred_element_type=F32)


def dot_nn(a, b):
    return jnp.dot(a, b, preferred_element_type=F32)


def kernel(
    rate_scale,
    q_ref, k_ref, v_ref, rates_ref, fast_ref, mom_ref, wout_ref,
    out_ref,
    gsrc, kbuf, gbuf, qbuf, wf, wb, mom, grad,
    csend, crecv, zsend, zrecv, normed, cscale,
    osend, obuf, wout, stash, total, msend, mrecv, fsend, frecv,
    a2a_send, a2a_recv, loc_sem, w_send, w_recv, cs_sem, cr_sem, zs_sem, zr_sem,
    ns_sem, nr_sem, ps_sem, pr_sem, os_sem, or_sem, ms_sem, mr_sem, fs_sem, fr_sem, wo_send, wo_recv,
):
    head, ctx = lax.axis_index("head"), lax.axis_index("ctx")
    x, c = head // 2, head % 2
    z, y = ctx // 4, ctx % 4
    owner = y // 2
    local = y % 2

    def dev(dx=0, dy=0, dz=0, dc=0):
        return (((x + dx) % 4) * 2 + (c + dc) % 2, ((z + dz) % 4) * 4 + (y + dy) % 4)

    def remote(src, dst, ssem, rsem, where):
        return pltpu.make_async_remote_copy(
            src_ref=src, dst_ref=dst, send_sem=ssem, recv_sem=rsem, device_id=where, device_id_type=MESH
        )

    barrier = pltpu.get_barrier_semaphore()
    for dx, dy in K_OFFSETS[1:]:
        pl.semaphore_signal(barrier, inc=1, device_id=dev(dx, dy), device_id_type=MESH)
    for dz in (1, 2, 3):
        pl.semaphore_signal(barrier, inc=1, device_id=dev(dz=dz), device_id_type=MESH)
    pl.semaphore_signal(barrier, inc=1, device_id=dev(dc=1), device_id_type=MESH)

    scaled = -(rates_ref[...].T * rate_scale)
    for h in range(16):
        cols = pl.ds(h * 256, 256)
        gsrc[:, cols] = (scaled[:, h : h + 1] * v_ref[:, cols].astype(F32)).astype(BF16)

    mine = pl.multiple_of((x * 4 + y) * 256, 256)
    k_own = pltpu.make_async_copy(k_ref.at[:, pl.ds(mine, 256)], kbuf.at[pl.ds(0, 128)], a2a_recv.at[0, 0])
    q_own = pltpu.make_async_copy(q_ref.at[:, pl.ds(mine, 256)], qbuf.at[pl.ds(0, 128)], a2a_recv.at[2, 0])
    k_own.start()
    gbuf[pl.ds(0, 128), :] = gsrc[:, pl.ds(mine, 256)]

    pl.semaphore_wait(barrier, 19)

    def block_copy(kind, source, target, slot):
        dx, dy = (Q_OFFSETS if kind == 2 else K_OFFSETS)[slot]
        to = pl.multiple_of((((x + dx) % 4) * 4 + (y + dy) % 4) * 256, 256)
        return remote(
            source.at[:, pl.ds(to, 256)], target.at[pl.ds(slot * 128, 128)],
            a2a_send.at[kind, slot], a2a_recv.at[kind, slot], dev(dx, dy),
        )

    def weights_in(m):
        return pltpu.make_async_copy(fast_ref.at[local, m], wf.at[m], loc_sem.at[m])

    def weights_over(m):
        return remote(fast_ref.at[local, m], wf.at[m], w_send.at[m], w_recv.at[m], dev(dc=1))

    row_own = pl.multiple_of(c * 512 + z * 128, 128)
    row_other = pl.multiple_of((1 - c) * 512 + z * 128, 128)
    mom_in = pltpu.make_async_copy(mom_ref.at[local, :, pl.ds(row_own, 128)], mom, loc_sem.at[3])
    mom_over = remote(mom_ref.at[local, :, pl.ds(row_other, 128)], mom, w_send.at[3], w_recv.at[3], dev(dc=1))

    a2a = []

    def send_group(slots):
        for slot in slots:
            for kind, source, target in ((0, k_ref, kbuf), (1, gsrc, gbuf)):
                copy = block_copy(kind, source, target, slot)
                copy.start()
                a2a.append(copy)

    send_group((1, 2, 3, 4))

    @pl.when(c == owner)
    def _():
        for m in range(3):
            weights_over(m).start()
            weights_in(m).start()
        mom_over.start()
        mom_in.start()

    send_group(range(5, 16))

    for m in range(3):
        @pl.when(c == owner)
        def _():
            weights_in(m).wait()

        @pl.when(c != owner)
        def _():
            weights_over(m).wait_recv()

        wb[m] = wf[m].astype(BF16)

    chunk = 512

    def grad_block(t, first):
        toks = pl.ds(pl.multiple_of(t * 256, 256), 256)

        def body(i, carry):
            rows = pl.ds(pl.multiple_of(i * chunk, chunk), chunk)
            keys, gout = kbuf[toks, :], gbuf[toks, :]
            pre = dot_nt(wb[0, rows, :], keys)
            gate = dot_nt(wb[1, rows, :], keys)
            back = dot_nt(wb[2, rows, :], gout)
            sg = 0.5 + 0.5 * jnp.tanh(0.5 * pre)
            silu = pre * sg
            hidden = (silu * gate).astype(BF16)
            grad_gate = (back * silu).astype(BF16)
            grad_pre = ((back * gate) * (sg + silu - silu * sg)).astype(BF16)
            g0 = dot_nn(grad_pre, keys)
            g1 = dot_nn(grad_gate, keys)
            g2 = dot_nn(hidden, gout)
            if first:
                grad[0, rows, :] = g0
                grad[1, rows, :] = g1
                grad[2, rows, :] = g2
            else:
                grad[0, rows, :] += g0
                grad[1, rows, :] += g1
                grad[2, rows, :] += g2
            return carry

        lax.fori_loop(0, 1024 // chunk, body, 0)

    def slot_wait(kind, target, slot):
        remote(
            target.at[pl.ds(0, 128)], target.at[pl.ds(slot * 128, 128)],
            a2a_send.at[kind, slot], a2a_recv.at[kind, slot], dev(1),
        ).wait_recv()

    k_own.wait()
    for t in range(8):
        for slot in (2 * t, 2 * t + 1):
            if slot > 0:
                slot_wait(0, kbuf, slot)
                slot_wait(1, gbuf, slot)
        if t == 7:
            for slot in Q_ORDER:
                copy = block_copy(2, q_ref, qbuf, slot)
                copy.start()
                a2a.append(copy)
            q_own.start()
        grad_block(t, t == 0)

    wo_rows = pl.ds(pl.multiple_of(c * 512, 512), 512)
    wo_in = pltpu.make_async_copy(wout_ref, wout.at[wo_rows], loc_sem.at[4])
    wo_over = remote(wout_ref, wout.at[wo_rows], wo_send, wo_recv, dev(dc=1))

    core_copies = []
    for n, dz in enumerate((2, 1, 3, 0)):
        rows = pl.ds(pl.multiple_of((1 - c) * 512 + ((z + dz) % 4) * 128, 128), 128)
        csend[n] = grad[:, rows, :].astype(BF16)
        copy = remote(csend.at[n], crecv.at[n], cs_sem.at[n], cr_sem.at[n], dev(dc=1))
        copy.start()
        core_copies.append(copy)
    z_copies = []
    for n, dz in enumerate((2, 1, 3)):
        rows = pl.ds(pl.multiple_of(c * 512 + ((z + dz) % 4) * 128, 128), 128)
        core_copies[n].wait_recv()
        zsend[n] = (grad[:, rows, :] + crecv[n].astype(F32)).astype(BF16)
        copy = remote(zsend.at[n], zrecv.at[n], zs_sem.at[n], zr_sem.at[n], dev(dz=dz))
        copy.start()
        z_copies.append(copy)
    wo_in.start()
    wo_over.start()
    core_copies[3].wait_recv()
    own = pl.ds(row_own, 128)

    @pl.when(c == owner)
    def _():
        mom_in.wait()

    @pl.when(c != owner)
    def _():
        mom_over.wait_recv()

    base = wf[:, own, :] - 0.9 * mom[...] - (grad[:, own, :] + crecv[3].astype(F32))
    grad[:, own, :] = base
    row_old = jnp.sqrt(jnp.sum(jnp.square(wf[0:2, own, :]), axis=2, keepdims=True))
    column_old = jnp.sqrt(jnp.sum(jnp.square(wf[2]), axis=0, keepdims=True))
    for n in range(3):
        z_copies[n].wait_recv()
    updated = grad[:, own, :] - (zrecv[0].astype(F32) + zrecv[1].astype(F32) + zrecv[2].astype(F32))
    row_new = jnp.sum(jnp.square(updated[0:2]), axis=2, keepdims=True)
    normed[0:2, own, :] = (updated[0:2] * row_old / jnp.sqrt(row_new + 1e-06)).astype(BF16)
    normed[2, own, :] = updated[2].astype(BF16)

    n_copies, p_copies = [], []
    for n, dz in enumerate((2, 1, 3)):
        copy = remote(normed.at[:, own], normed.at[:, own], ns_sem.at[n], nr_sem.at[n], dev(dz=dz))
        copy.start()
        n_copies.append(copy)
    copy = remote(normed.at[:, own], normed.at[:, own], ps_sem.at[3], pr_sem.at[3], dev(dc=1))
    copy.start()
    p_copies.append(copy)
    for n, dz in ((1, 1), (2, 3), (0, 2)):
        n_copies[n].wait_recv()
        rows = pl.ds(pl.multiple_of(c * 512 + ((z - dz) % 4) * 128, 128), 128)
        copy = remote(normed.at[:, rows], normed.at[:, rows], ps_sem.at[n], pr_sem.at[n], dev(dc=1))
        copy.start()
        p_copies.append(copy)
    for copy in p_copies:
        copy.wait_recv()
    column_new = jnp.sum(jnp.square(normed[2].astype(F32)), axis=0, keepdims=True)
    cscale[...] = column_old / jnp.sqrt(column_new + 1e-06)

    q_own.wait()

    def apply_slots(t):
        toks = pl.ds(t * 256, 256)

        def body(i, acc):
            rows = pl.ds(pl.multiple_of(i * chunk, chunk), chunk)
            query = qbuf[toks, :]
            pre = dot_nt(query, normed[0, rows, :])
            gate = dot_nt(query, normed[1, rows, :])
            hidden = (pre * (0.5 + 0.5 * jnp.tanh(0.5 * pre)) * gate).astype(BF16)
            return acc + dot_nn(hidden, normed[2, rows, :])

        acc = lax.fori_loop(0, 1024 // chunk, body, jnp.zeros((256, 256), F32))
        osend[toks, :] = (acc * cscale[...]).astype(BF16)

    my_cols = pl.ds(pl.multiple_of(y * 256, 256), 256)
    o_copies = []

    def apply_blocks(*blocks):
        for t in blocks:
            for slot in (2 * t, 2 * t + 1):
                if slot > 0:
                    slot_wait(2, qbuf, slot)
            apply_slots(t)
            for slot in (2 * t, 2 * t + 1):
                dx, dy = Q_OFFSETS[slot]
                if dy == 0:
                    obuf[pl.ds(dx * 128, 128), my_cols] = osend[pl.ds(slot * 128, 128), :]
                else:
                    copy = remote(
                        osend.at[pl.ds(slot * 128, 128)], obuf.at[pl.ds(dx * 128, 128), my_cols],
                        os_sem.at[dx, dy], or_sem.at[dx, dy], dev(dy=-dy),
                    )
                    copy.start()
                    o_copies.append(copy)

    def apply_far(half):
        def body(i, acc):
            rows = pl.ds(pl.multiple_of(i * chunk, chunk), chunk)
            query = jnp.concatenate([qbuf[pl.ds(slot * 128 + half * 64, 64), :] for slot in range(4, 8)], axis=0)
            pre = dot_nt(query, normed[0, rows, :])
            gate = dot_nt(query, normed[1, rows, :])
            hidden = (pre * (0.5 + 0.5 * jnp.tanh(0.5 * pre)) * gate).astype(BF16)
            return acc + dot_nn(hidden, normed[2, rows, :])

        acc = lax.fori_loop(0, 1024 // chunk, body, jnp.zeros((256, 256), F32))
        result = (acc * cscale[...]).astype(BF16)
        obuf[pl.ds(256 + half * 64, 64), my_cols] = result[0:64]
        for n in (3, 1, 2):
            rows = pl.ds((4 + n) * 128 + half * 64, 64)
            osend[rows, :] = result[n * 64 : n * 64 + 64]
            dy = Q_OFFSETS[4 + n][1]
            copy = remote(
                osend.at[rows], obuf.at[pl.ds(256 + half * 64, 64), my_cols],
                os_sem.at[2 + 2 * half, dy], or_sem.at[2 + 2 * half, dy], dev(dy=-dy),
            )
            copy.start()
            o_copies.append(copy)

    for slot in range(4, 8):
        slot_wait(2, qbuf, slot)
    apply_far(0)
    apply_far(1)
    apply_blocks(4, 5)

    wo_in.wait()
    wo_over.wait_recv()

    def o_wait(dx, rows=128):
        for dy in (1, 2, 3):
            remote(
                osend.at[pl.ds(0, rows)], obuf.at[pl.ds(0, rows), pl.ds(0, 256)],
                os_sem.at[dx, dy], or_sem.at[dx, dy], dev(1),
            ).wait_recv()

    def message(kind, j, up):
        return remote(
            msend.at[kind, j], mrecv.at[kind, j], ms_sem.at[kind, j], mr_sem.at[kind, j], dev(1 if up else -1)
        )

    def product(first, rows, j, width=512):
        return dot_nn(obuf[pl.ds(first, rows), :], wout[:, pl.ds(pl.multiple_of(j * width, width), width)])

    def far_message(kind, part):
        return remote(
            fsend.at[kind, part], frecv.at[kind, part], fs_sem.at[kind, part], fr_sem.at[kind, part],
            dev(-1 if kind else 1),
        )

    for half in (0, 1):
        o_wait(2 + 2 * half, 64)

        def far(n, carry):
            j, kind = n // 2, n % 2
            fsend[kind, 2 * half + j] = product(256 + half * 64, 64, j + 2 * kind, 1024).astype(BF16)
            far_message(kind, 2 * half + j).start()
            return carry

        for n in range(4):
            far(n, 0)
    apply_blocks(6, 7, 1, 0)
    o_wait(1)
    o_wait(3)

    def near(j, carry):
        msend[0, j] = product(384, 128, j + 4).astype(BF16)
        message(0, j, True).start()
        msend[1, j] = product(128, 128, j).astype(BF16)
        message(1, j, False).start()
        return carry

    lax.fori_loop(0, 4, near, 0)

    def relay_part(j, carry):
        stash[0, j] = product(384, 128, j)
        stash[1, j] = product(128, 128, j + 4)
        return carry

    lax.fori_loop(0, 4, relay_part, 0)

    for j in range(4):
        for kind in (0, 1):
            if j % 2 == 0:
                far_message(kind, j // 2).wait_recv()
                far_message(kind, 2 + j // 2).wait_recv()
            for half in (0, 1):
                rows, cols = pl.ds(half * 64, 64), pl.ds((j % 2) * 512, 512)
                msend[2 + kind, j, rows, :] = (
                    stash[kind, j, rows, :] + frecv[kind, 2 * half + j // 2, :, cols].astype(F32)
                ).astype(BF16)
            message(2 + kind, j, kind == 0).start()

    o_wait(0)

    def rest(j, carry):
        total[j] = product(0, 128, j)
        return carry

    lax.fori_loop(0, 8, rest, 0)

    def finish(j, carry):
        low = pl.ds(pl.multiple_of(j * 512, 512), 512)
        high = pl.ds(pl.multiple_of(j * 512 + 2048, 512), 512)
        message(1, j, False).wait_recv()
        message(0, j, True).wait_recv()
        message(2, j, True).wait_recv()
        out_ref[:, low] = (total[j] + mrecv[1, j].astype(F32) + mrecv[2, j].astype(F32)).astype(BF16)
        message(3, j, False).wait_recv()
        out_ref[:, high] = (total[j + 4] + mrecv[0, j].astype(F32) + mrecv[3, j].astype(F32)).astype(BF16)
        return carry

    lax.fori_loop(0, 4, finish, 0)

    for copy in a2a + core_copies + z_copies + n_copies + p_copies + o_copies:
        copy.wait_send()
    wo_over.wait_send()

    @pl.when(c == owner)
    def _():
        for m in range(3):
            weights_over(m).wait_send()
        mom_over.wait_send()

    def drain(j, carry):
        for kind in range(4):
            message(kind, j, kind % 2 == 0).wait_send()
        for kind in range(2):
            far_message(kind, j).wait_send()
        return carry

    lax.fori_loop(0, 4, drain, 0)


def shards(query_rows, key_rows, value_rows, token_rates, fast_weights, momentum, out_weight):
    tokens = key_rows.shape[0] * lax.axis_size("head") * lax.axis_size("ctx")
    anywhere = pl.BlockSpec(memory_space=pl.ANY)
    vmem = pl.BlockSpec(memory_space=pltpu.VMEM)
    dma = pltpu.SemaphoreType.DMA
    return pl.pallas_call(
        functools.partial(kernel, float(tokens) ** (-0.5)),
        out_shape=pltpu.VMEM((128, 4096), BF16),
        in_specs=[anywhere, anywhere, vmem, vmem, anywhere, anywhere, anywhere],
        out_specs=vmem,
        scratch_shapes=[
            pltpu.VMEM((128, 4096), BF16),
            pltpu.VMEM((2048, 256), BF16),
            pltpu.VMEM((2048, 256), BF16),
            pltpu.VMEM((2048, 256), BF16),
            pltpu.VMEM((3, 1024, 256), F32),
            pltpu.VMEM((3, 1024, 256), BF16),
            pltpu.VMEM((3, 128, 256), F32),
            pltpu.VMEM((3, 1024, 256), F32),
            pltpu.VMEM((4, 3, 128, 256), BF16),
            pltpu.VMEM((4, 3, 128, 256), BF16),
            pltpu.VMEM((3, 3, 128, 256), BF16),
            pltpu.VMEM((3, 3, 128, 256), BF16),
            pltpu.VMEM((3, 1024, 256), BF16),
            pltpu.VMEM((1, 256), F32),
            pltpu.VMEM((2048, 256), BF16),
            pltpu.VMEM((512, 1024), BF16),
            pltpu.VMEM((1024, 4096), BF16),
            pltpu.VMEM((2, 4, 128, 512), F32),
            pltpu.VMEM((8, 128, 512), F32),
            pltpu.VMEM((4, 4, 128, 512), BF16),
            pltpu.VMEM((4, 4, 128, 512), BF16),
            pltpu.VMEM((2, 4, 64, 1024), BF16),
            pltpu.VMEM((2, 4, 64, 1024), BF16),
            dma((3, 16)), dma((3, 16)), dma((5,)), dma((4,)), dma((4,)), dma((4,)), dma((4,)), dma((3,)), dma((3,)),
            dma((3,)), dma((3,)), dma((4,)), dma((4,)), dma((5, 4)), dma((5, 4)), dma((4, 4)), dma((4, 4)),
            dma((2, 4)), dma((2, 4)), dma(()), dma(()),
        ],
        compiler_params=pltpu.CompilerParams(collective_id=0, has_side_effects=True, vmem_limit_bytes=62 * 2**20),
        name="ttt_layer",
    )(query_rows, key_rows, value_rows, token_rates.T, fast_weights, momentum, out_weight)


def solution(mesh):
    placed = (
        P(("head", "ctx"), None),
        P(("head", "ctx"), None),
        P(("head", "ctx"), None),
        P(("head", "ctx"), None),
        P("head", None, None, None),
        P("head", None, None, None),
        P("head", None),
    )
    return jax.shard_map(
        shards, mesh=mesh, in_specs=placed, out_specs=P(("head", "ctx"), None), check_vma=False
    )
```

```python
import functools

import jax
import jax.numpy as jnp
from jax import lax
from jax.experimental import pallas as pl
from jax.experimental.pallas import tpu as pltpu
from jax.sharding import PartitionSpec as P

MESH = pl.DeviceIdType.MESH
F32 = jnp.float32
BF16 = jnp.bfloat16

K_OFFSETS = (
    (0, 0), (2, 2), (1, 1), (3, 3),
    (2, 1), (1, 2), (2, 3), (3, 2),
    (2, 0), (0, 2), (1, 3), (3, 1),
    (1, 0), (0, 1), (3, 0), (0, 3),
)
Q_OFFSETS = (
    (0, 0), (0, 1), (0, 3), (0, 2),
    (2, 0), (2, 1), (2, 3), (2, 2),
    (1, 2), (3, 2), (1, 1), (3, 3),
    (1, 3), (3, 1), (1, 0), (3, 0),
)
Q_ORDER = (7, 10, 11, 5, 8, 6, 9, 4, 3, 12, 13, 14, 1, 15, 2)


NT = (((1,), (1,)), ((), ()))


def dot_nt(a, b):
    return lax.dot_general(a, b, NT, preferred_element_type=F32)


def dot_nn(a, b):
    return jnp.dot(a, b, preferred_element_type=F32)


def kernel(
    rate_scale,
    q_ref, k_ref, v_ref, rates_ref, fast_ref, mom_ref, wout_ref,
    out_ref,
    gsrc, kbuf, gbuf, qbuf, wf, wb, mom, grad,
    csend, crecv, zsend, zrecv, normed, cscale,
    osend, obuf, wout, stash, total, msend, mrecv, fsend, frecv,
    a2a_send, a2a_recv, loc_sem, w_send, w_recv, cs_sem, cr_sem, zs_sem, zr_sem,
    ns_sem, nr_sem, ps_sem, pr_sem, os_sem, or_sem, ms_sem, mr_sem, fs_sem, fr_sem, wo_send, wo_recv,
):
    head, ctx = lax.axis_index("head"), lax.axis_index("ctx")
    x, c = head // 2, head % 2
    z, y = ctx // 4, ctx % 4
    owner = y // 2
    local = y % 2

    def dev(dx=0, dy=0, dz=0, dc=0):
        return (((x + dx) % 4) * 2 + (c + dc) % 2, ((z + dz) % 4) * 4 + (y + dy) % 4)

    def remote(src, dst, ssem, rsem, where):
        return pltpu.make_async_remote_copy(
            src_ref=src, dst_ref=dst, send_sem=ssem, recv_sem=rsem, device_id=where, device_id_type=MESH
        )

    barrier = pltpu.get_barrier_semaphore()
    for dx, dy in K_OFFSETS[1:]:
        pl.semaphore_signal(barrier, inc=1, device_id=dev(dx, dy), device_id_type=MESH)
    for dz in (1, 2, 3):
        pl.semaphore_signal(barrier, inc=1, device_id=dev(dz=dz), device_id_type=MESH)
    pl.semaphore_signal(barrier, inc=1, device_id=dev(dc=1), device_id_type=MESH)

    scaled = -(rates_ref[...].T * rate_scale)
    for h in range(16):
        cols = pl.ds(h * 256, 256)
        gsrc[:, cols] = (scaled[:, h : h + 1] * v_ref[:, cols].astype(F32)).astype(BF16)

    mine = pl.multiple_of((x * 4 + y) * 256, 256)
    k_own = pltpu.make_async_copy(k_ref.at[:, pl.ds(mine, 256)], kbuf.at[pl.ds(0, 128)], a2a_recv.at[0, 0])
    q_own = pltpu.make_async_copy(q_ref.at[:, pl.ds(mine, 256)], qbuf.at[pl.ds(0, 128)], a2a_recv.at[2, 0])
    k_own.start()
    gbuf[pl.ds(0, 128), :] = gsrc[:, pl.ds(mine, 256)]
    grad[...] = jnp.zeros_like(grad)

    pl.semaphore_wait(barrier, 19)

    def block_copy(kind, source, target, slot):
        dx, dy = (Q_OFFSETS if kind == 2 else K_OFFSETS)[slot]
        to = pl.multiple_of((((x + dx) % 4) * 4 + (y + dy) % 4) * 256, 256)
        return remote(
            source.at[:, pl.ds(to, 256)], target.at[pl.ds(slot * 128, 128)],
            a2a_send.at[kind, slot], a2a_recv.at[kind, slot], dev(dx, dy),
        )

    def weights_in(m):
        return pltpu.make_async_copy(fast_ref.at[local, m], wf.at[m], loc_sem.at[m])

    def weights_over(m):
        return remote(fast_ref.at[local, m], wf.at[m], w_send.at[m], w_recv.at[m], dev(dc=1))

    row_own = pl.multiple_of(c * 512 + z * 128, 128)
    row_other = pl.multiple_of((1 - c) * 512 + z * 128, 128)
    mom_in = pltpu.make_async_copy(mom_ref.at[local, :, pl.ds(row_own, 128)], mom, loc_sem.at[3])
    mom_over = remote(mom_ref.at[local, :, pl.ds(row_other, 128)], mom, w_send.at[3], w_recv.at[3], dev(dc=1))

    a2a = []

    def send_group(slots):
        for slot in slots:
            for kind, source, target in ((0, k_ref, kbuf), (1, gsrc, gbuf)):
                copy = block_copy(kind, source, target, slot)
                copy.start()
                a2a.append(copy)

    send_group((1, 2, 3, 4))

    @pl.when(c == owner)
    def _():
        for m in range(3):
            weights_over(m).start()
            weights_in(m).start()
        mom_over.start()
        mom_in.start()

    send_group(range(5, 16))

    for m in range(3):
        @pl.when(c == owner)
        def _():
            weights_in(m).wait()

        @pl.when(c != owner)
        def _():
            weights_over(m).wait_recv()

        wb[m] = wf[m].astype(BF16)

    def grad_block(start, size):
        toks = pl.ds(pl.multiple_of(start, 256), size)
        keys, gout = kbuf[toks, :], gbuf[toks, :]
        pre = dot_nt(wb[0], keys)
        gate = dot_nt(wb[1], keys)
        back = dot_nt(wb[2], gout)
        sg = 0.5 + 0.5 * jnp.tanh(0.5 * pre)
        silu = pre * sg
        hidden = (silu * gate).astype(BF16)
        grad_gate = (back * silu).astype(BF16)
        grad_pre = ((back * gate) * (sg + silu - silu * sg)).astype(BF16)
        grad[0] += dot_nn(grad_pre, keys)
        grad[1] += dot_nn(grad_gate, keys)
        grad[2] += dot_nn(hidden, gout)

    def slot_wait(kind, target, slot):
        remote(
            target.at[pl.ds(0, 128)], target.at[pl.ds(slot * 128, 128)],
            a2a_send.at[kind, slot], a2a_recv.at[kind, slot], dev(1),
        ).wait_recv()

    k_own.wait()

    def block(t, carry):
        @pl.when(t > 0)
        def _():
            slot_wait(0, kbuf, 2 * t)
            slot_wait(1, gbuf, 2 * t)

        slot_wait(0, kbuf, 2 * t + 1)
        slot_wait(1, gbuf, 2 * t + 1)
        grad_block(t * 256, 256)
        return carry

    lax.fori_loop(0, 6, block, 0)
    for slot in range(12, 16):
        slot_wait(0, kbuf, slot)
        slot_wait(1, gbuf, slot)
    for slot in Q_ORDER:
        copy = block_copy(2, q_ref, qbuf, slot)
        copy.start()
        a2a.append(copy)
    q_own.start()
    grad_block(1536, 512)

    wo_rows = pl.ds(pl.multiple_of(c * 512, 512), 512)
    wo_in = pltpu.make_async_copy(wout_ref, wout.at[wo_rows], loc_sem.at[4])
    wo_over = remote(wout_ref, wout.at[wo_rows], wo_send, wo_recv, dev(dc=1))

    core_copies = []
    for n, dz in enumerate((2, 1, 3, 0)):
        rows = pl.ds(pl.multiple_of((1 - c) * 512 + ((z + dz) % 4) * 128, 128), 128)
        csend[n] = grad[:, rows, :].astype(BF16)
        copy = remote(csend.at[n], crecv.at[n], cs_sem.at[n], cr_sem.at[n], dev(dc=1))
        copy.start()
        core_copies.append(copy)
    z_copies = []

    def piece(n, dz, part):
        rows = pl.ds(pl.multiple_of(c * 512 + ((z + dz) % 4) * 128 + part * 64, 64), 64)
        return grad[:, rows, :] + crecv[n, :, pl.ds(part * 64, 64), :].astype(F32)

    def z_send(n, value, dz):
        zsend[n] = value.astype(BF16)
        copy = remote(zsend.at[n], zrecv.at[n], zs_sem.at[n], zr_sem.at[n], dev(dz=dz))
        copy.start()
        z_copies.append(copy)

    core_copies[0].wait_recv()
    z_send(0, piece(0, 2, 0), 1)
    z_send(1, piece(0, 2, 1), -1)
    core_copies[1].wait_recv()
    z_send(2, piece(1, 1, 1), 1)
    core_copies[2].wait_recv()
    z_send(3, piece(2, 3, 0), -1)
    z_copies[0].wait_recv()
    z_send(4, piece(1, 1, 0) + zrecv[0].astype(F32), 1)
    z_copies[1].wait_recv()
    z_send(5, piece(2, 3, 1) + zrecv[1].astype(F32), -1)
    wo_in.start()
    wo_over.start()
    core_copies[3].wait_recv()
    own = pl.ds(row_own, 128)

    @pl.when(c == owner)
    def _():
        mom_in.wait()

    @pl.when(c != owner)
    def _():
        mom_over.wait_recv()

    base = wf[:, own, :] - 0.9 * mom[...] - (grad[:, own, :] + crecv[3].astype(F32))
    grad[:, own, :] = base
    row_old = jnp.sqrt(jnp.sum(jnp.square(wf[0:2, own, :]), axis=2, keepdims=True))
    column_old = jnp.sqrt(jnp.sum(jnp.square(wf[2]), axis=0, keepdims=True))
    for n in range(2, 6):
        z_copies[n].wait_recv()
    others = jnp.concatenate(
        [zrecv[4].astype(F32) + zrecv[3].astype(F32), zrecv[2].astype(F32) + zrecv[5].astype(F32)], axis=1
    )
    updated = grad[:, own, :] - others
    row_new = jnp.sum(jnp.square(updated[0:2]), axis=2, keepdims=True)
    normed[0:2, own, :] = (updated[0:2] * row_old / jnp.sqrt(row_new + 1e-06)).astype(BF16)
    normed[2, own, :] = updated[2].astype(BF16)

    def half_rows(dz, part):
        return pl.ds(pl.multiple_of(c * 512 + ((z + dz) % 4) * 128 + part * 64, 64), 64)

    n_copies, p_copies = [], []

    def n_send(n, rows, dz):
        copy = remote(normed.at[:, rows], normed.at[:, rows], ns_sem.at[n], nr_sem.at[n], dev(dz=dz))
        copy.start()
        n_copies.append(copy)

    def p_send(n, rows):
        copy = remote(normed.at[:, rows], normed.at[:, rows], ps_sem.at[n], pr_sem.at[n], dev(dc=1))
        copy.start()
        p_copies.append(copy)

    n_send(0, half_rows(0, 0), 1)
    n_send(1, half_rows(0, 1), -1)
    n_send(2, half_rows(0, 1), 1)
    n_send(3, half_rows(0, 0), -1)
    p_send(6, own)
    n_copies[0].wait_recv()
    n_send(4, half_rows(-1, 0), 1)
    p_send(0, half_rows(-1, 0))
    n_copies[1].wait_recv()
    n_send(5, half_rows(1, 1), -1)
    p_send(1, half_rows(1, 1))
    for n, dz, part in ((2, -1, 1), (3, 1, 0), (4, 2, 0), (5, 2, 1)):
        n_copies[n].wait_recv()
        p_send(n, half_rows(dz, part))
    for copy in p_copies:
        copy.wait_recv()
    column_new = jnp.sum(jnp.square(normed[2].astype(F32)), axis=0, keepdims=True)
    cscale[...] = column_old / jnp.sqrt(column_new + 1e-06)

    q_own.wait()

    def applied(query):
        hidden = []
        for i in range(4):
            rows = pl.ds(i * 256, 256)
            pre = dot_nt(query, normed[0, rows, :])
            gate = dot_nt(query, normed[1, rows, :])
            hidden.append((pre * (0.5 + 0.5 * jnp.tanh(0.5 * pre)) * gate).astype(BF16))
        return (dot_nn(jnp.concatenate(hidden, axis=1), normed[2]) * cscale[...]).astype(BF16)

    my_cols = pl.ds(pl.multiple_of(y * 256, 256), 256)
    o_copies = []

    def apply_group(first):
        for slot in range(first, first + 4):
            if slot > 0:
                slot_wait(2, qbuf, slot)
        osend[pl.ds(first * 128, 512), :] = applied(qbuf[pl.ds(first * 128, 512), :])
        for slot in range(first, first + 4):
            dx, dy = Q_OFFSETS[slot]
            if dy == 0:
                obuf[pl.ds(dx * 128, 128), my_cols] = osend[pl.ds(slot * 128, 128), :]
            else:
                copy = remote(
                    osend.at[pl.ds(slot * 128, 128)], obuf.at[pl.ds(dx * 128, 128), my_cols],
                    os_sem.at[dx, dy], or_sem.at[dx, dy], dev(dy=-dy),
                )
                copy.start()
                o_copies.append(copy)

    def apply_far(half):
        result = applied(
            jnp.concatenate([qbuf[pl.ds(slot * 128 + half * 64, 64), :] for slot in range(4, 8)], axis=0)
        )
        obuf[pl.ds(256 + half * 64, 64), my_cols] = result[0:64]
        for n in (3, 1, 2):
            rows = pl.ds((4 + n) * 128 + half * 64, 64)
            osend[rows, :] = result[n * 64 : n * 64 + 64]
            dy = Q_OFFSETS[4 + n][1]
            copy = remote(
                osend.at[rows], obuf.at[pl.ds(256 + half * 64, 64), my_cols],
                os_sem.at[2 + 2 * half, dy], or_sem.at[2 + 2 * half, dy], dev(dy=-dy),
            )
            copy.start()
            o_copies.append(copy)

    for slot in range(4, 8):
        slot_wait(2, qbuf, slot)
    apply_far(0)
    apply_far(1)
    apply_group(8)

    wo_in.wait()
    wo_over.wait_recv()

    def o_wait(dx, rows=128):
        for dy in (1, 2, 3):
            remote(
                osend.at[pl.ds(0, rows)], obuf.at[pl.ds(0, rows), pl.ds(0, 256)],
                os_sem.at[dx, dy], or_sem.at[dx, dy], dev(1),
            ).wait_recv()

    def message(kind, j, up):
        return remote(
            msend.at[kind, j], mrecv.at[kind, j], ms_sem.at[kind, j], mr_sem.at[kind, j], dev(1 if up else -1)
        )

    def product(first, rows, j, width=512):
        return dot_nn(obuf[pl.ds(first, rows), :], wout[:, pl.ds(pl.multiple_of(j * width, width), width)])

    def far_message(kind, part):
        return remote(
            fsend.at[kind, part], frecv.at[kind, part], fs_sem.at[kind, part], fr_sem.at[kind, part],
            dev(-1 if kind else 1),
        )

    for half in (0, 1):
        o_wait(2 + 2 * half, 64)

        def far(n, carry):
            j, kind = n // 2, n % 2
            fsend[kind, 2 * half + j] = product(256 + half * 64, 64, j + 2 * kind, 1024).astype(BF16)
            far_message(kind, 2 * half + j).start()
            return carry

        for n in range(4):
            far(n, 0)
    apply_group(12)
    apply_group(0)
    o_wait(1)
    o_wait(3)

    def near(j, carry):
        msend[0, j] = product(384, 128, j + 4).astype(BF16)
        message(0, j, True).start()
        msend[1, j] = product(128, 128, j).astype(BF16)
        message(1, j, False).start()
        return carry

    lax.fori_loop(0, 4, near, 0)

    def relay_part(j, carry):
        stash[0, j] = product(384, 128, j)
        stash[1, j] = product(128, 128, j + 4)
        return carry

    lax.fori_loop(0, 4, relay_part, 0)

    for j in range(4):
        for kind in (0, 1):
            if j % 2 == 0:
                far_message(kind, j // 2).wait_recv()
                far_message(kind, 2 + j // 2).wait_recv()
            for half in (0, 1):
                rows, cols = pl.ds(half * 64, 64), pl.ds((j % 2) * 512, 512)
                msend[2 + kind, j, rows, :] = (
                    stash[kind, j, rows, :] + frecv[kind, 2 * half + j // 2, :, cols].astype(F32)
                ).astype(BF16)
            message(2 + kind, j, kind == 0).start()

    o_wait(0)

    def rest(j, carry):
        total[j] = product(0, 128, j)
        return carry

    lax.fori_loop(0, 8, rest, 0)

    def finish(j, carry):
        low = pl.ds(pl.multiple_of(j * 512, 512), 512)
        high = pl.ds(pl.multiple_of(j * 512 + 2048, 512), 512)
        message(1, j, False).wait_recv()
        message(0, j, True).wait_recv()
        message(2, j, True).wait_recv()
        out_ref[:, low] = (total[j] + mrecv[1, j].astype(F32) + mrecv[2, j].astype(F32)).astype(BF16)
        message(3, j, False).wait_recv()
        out_ref[:, high] = (total[j + 4] + mrecv[0, j].astype(F32) + mrecv[3, j].astype(F32)).astype(BF16)
        return carry

    lax.fori_loop(0, 4, finish, 0)

    for copy in a2a + core_copies + z_copies + n_copies + p_copies + o_copies:
        copy.wait_send()
    wo_over.wait_send()

    @pl.when(c == owner)
    def _():
        for m in range(3):
            weights_over(m).wait_send()
        mom_over.wait_send()

    def drain(j, carry):
        for kind in range(4):
            message(kind, j, kind % 2 == 0).wait_send()
        for kind in range(2):
            far_message(kind, j).wait_send()
        return carry

    lax.fori_loop(0, 4, drain, 0)


def shards(query_rows, key_rows, value_rows, token_rates, fast_weights, momentum, out_weight):
    tokens = key_rows.shape[0] * lax.axis_size("head") * lax.axis_size("ctx")
    anywhere = pl.BlockSpec(memory_space=pl.ANY)
    vmem = pl.BlockSpec(memory_space=pltpu.VMEM)
    dma = pltpu.SemaphoreType.DMA
    return pl.pallas_call(
        functools.partial(kernel, float(tokens) ** (-0.5)),
        out_shape=pltpu.VMEM((128, 4096), BF16),
        in_specs=[anywhere, anywhere, vmem, vmem, anywhere, anywhere, anywhere],
        out_specs=vmem,
        scratch_shapes=[
            pltpu.VMEM((128, 4096), BF16),
            pltpu.VMEM((2048, 256), BF16),
            pltpu.VMEM((2048, 256), BF16),
            pltpu.VMEM((2048, 256), BF16),
            pltpu.VMEM((3, 1024, 256), F32),
            pltpu.VMEM((3, 1024, 256), BF16),
            pltpu.VMEM((3, 128, 256), F32),
            pltpu.VMEM((3, 1024, 256), F32),
            pltpu.VMEM((4, 3, 128, 256), BF16),
            pltpu.VMEM((4, 3, 128, 256), BF16),
            pltpu.VMEM((6, 3, 64, 256), BF16),
            pltpu.VMEM((6, 3, 64, 256), BF16),
            pltpu.VMEM((3, 1024, 256), BF16),
            pltpu.VMEM((1, 256), F32),
            pltpu.VMEM((2048, 256), BF16),
            pltpu.VMEM((512, 1024), BF16),
            pltpu.VMEM((1024, 4096), BF16),
            pltpu.VMEM((2, 4, 128, 512), F32),
            pltpu.VMEM((8, 128, 512), F32),
            pltpu.VMEM((4, 4, 128, 512), BF16),
            pltpu.VMEM((4, 4, 128, 512), BF16),
            pltpu.VMEM((2, 4, 64, 1024), BF16),
            pltpu.VMEM((2, 4, 64, 1024), BF16),
            dma((3, 16)), dma((3, 16)), dma((5,)), dma((4,)), dma((4,)), dma((4,)), dma((4,)), dma((6,)), dma((6,)),
            dma((6,)), dma((6,)), dma((7,)), dma((7,)), dma((5, 4)), dma((5, 4)), dma((4, 4)), dma((4, 4)),
            dma((2, 4)), dma((2, 4)), dma(()), dma(()),
        ],
        compiler_params=pltpu.CompilerParams(collective_id=0, has_side_effects=True, vmem_limit_bytes=62 * 2**20),
        name="ttt_layer",
    )(query_rows, key_rows, value_rows, token_rates.T, fast_weights, momentum, out_weight)


def solution(mesh):
    placed = (
        P(("head", "ctx"), None),
        P(("head", "ctx"), None),
        P(("head", "ctx"), None),
        P(("head", "ctx"), None),
        P("head", None, None, None),
        P("head", None, None, None),
        P("head", None),
    )
    return jax.shard_map(
        shards, mesh=mesh, in_specs=placed, out_specs=P(("head", "ctx"), None), check_vma=False
    )
```

```python
import functools

import jax
import jax.numpy as jnp
from jax import lax
from jax.experimental import pallas as pl
from jax.experimental.pallas import tpu as pltpu
from jax.sharding import PartitionSpec as P

MESH = pl.DeviceIdType.MESH
F32 = jnp.float32
BF16 = jnp.bfloat16

K_OFFSETS = (
    (0, 0), (2, 2), (1, 1), (3, 3),
    (2, 1), (1, 2), (2, 3), (3, 2),
    (2, 0), (0, 2), (1, 3), (3, 1),
    (1, 0), (0, 1), (3, 0), (0, 3),
)
Q_OFFSETS = (
    (0, 0), (0, 1), (0, 3), (0, 2),
    (2, 0), (2, 1), (2, 3), (2, 2),
    (1, 2), (3, 2), (1, 1), (3, 3),
    (1, 3), (3, 1), (1, 0), (3, 0),
)
Q_ORDER = (7, 10, 11, 5, 8, 6, 9, 4, 3, 12, 13, 14, 1, 15, 2)


NT = (((1,), (1,)), ((), ()))


def dot_nt(a, b):
    return lax.dot_general(a, b, NT, preferred_element_type=F32)


def dot_nn(a, b):
    return jnp.dot(a, b, preferred_element_type=F32)


def kernel(
    rate_scale,
    q_ref, k_ref, v_ref, rates_ref, fast_ref, mom_ref, wout_ref,
    out_ref,
    vbuf, gsrc, kbuf, gbuf, qbuf, wf, wb, mom, grad,
    csend, crecv, zsend, zrecv, normed, cscale,
    osend, obuf, wout, stash, total, msend, mrecv, fsend, frecv,
    a2a_send, a2a_recv, loc_sem, w_send, w_recv, cs_sem, cr_sem, zs_sem, zr_sem,
    ns_sem, nr_sem, ps_sem, pr_sem, os_sem, or_sem, ms_sem, mr_sem, fs_sem, fr_sem, wo_send, wo_recv,
):
    head, ctx = lax.axis_index("head"), lax.axis_index("ctx")
    x, c = head // 2, head % 2
    z, y = ctx // 4, ctx % 4
    owner = y // 2
    local = y % 2

    def dev(dx=0, dy=0, dz=0, dc=0):
        return (((x + dx) % 4) * 2 + (c + dc) % 2, ((z + dz) % 4) * 4 + (y + dy) % 4)

    def remote(src, dst, ssem, rsem, where):
        return pltpu.make_async_remote_copy(
            src_ref=src, dst_ref=dst, send_sem=ssem, recv_sem=rsem, device_id=where, device_id_type=MESH
        )

    barrier = pltpu.get_barrier_semaphore()
    for dx, dy in K_OFFSETS[1:]:
        pl.semaphore_signal(barrier, inc=1, device_id=dev(dx, dy), device_id_type=MESH)
    for dz in (1, 2, 3):
        pl.semaphore_signal(barrier, inc=1, device_id=dev(dz=dz), device_id_type=MESH)
    pl.semaphore_signal(barrier, inc=1, device_id=dev(dc=1), device_id_type=MESH)

    v_in = pltpu.make_async_copy(v_ref, vbuf, loc_sem.at[5])
    v_in.start()
    mine = pl.multiple_of((x * 4 + y) * 256, 256)
    k_own = pltpu.make_async_copy(k_ref.at[:, pl.ds(mine, 256)], kbuf.at[pl.ds(0, 128)], a2a_recv.at[0, 0])
    q_own = pltpu.make_async_copy(q_ref.at[:, pl.ds(mine, 256)], qbuf.at[pl.ds(0, 128)], a2a_recv.at[2, 0])
    k_own.start()

    pl.semaphore_wait(barrier, 19)

    def block_copy(kind, source, target, slot):
        dx, dy = (Q_OFFSETS if kind == 2 else K_OFFSETS)[slot]
        to = pl.multiple_of((((x + dx) % 4) * 4 + (y + dy) % 4) * 256, 256)
        return remote(
            source.at[:, pl.ds(to, 256)], target.at[pl.ds(slot * 128, 128)],
            a2a_send.at[kind, slot], a2a_recv.at[kind, slot], dev(dx, dy),
        )

    def weights_in(m):
        return pltpu.make_async_copy(fast_ref.at[local, m], wf.at[m], loc_sem.at[m])

    def weights_over(m):
        return remote(fast_ref.at[local, m], wf.at[m], w_send.at[m], w_recv.at[m], dev(dc=1))

    row_own = pl.multiple_of(c * 512 + z * 128, 128)
    row_other = pl.multiple_of((1 - c) * 512 + z * 128, 128)
    mom_in = pltpu.make_async_copy(mom_ref.at[local, :, pl.ds(row_own, 128)], mom, loc_sem.at[3])
    mom_over = remote(mom_ref.at[local, :, pl.ds(row_other, 128)], mom, w_send.at[3], w_recv.at[3], dev(dc=1))

    a2a = []

    def send(kind, source, target, slots):
        for slot in slots:
            copy = block_copy(kind, source, target, slot)
            copy.start()
            a2a.append(copy)

    send(0, k_ref, kbuf, range(1, 5))

    @pl.when(c == owner)
    def _():
        for m in range(3):
            weights_in(m).start()
        mom_in.start()
        for m in range(3):
            weights_over(m).start()
        mom_over.start()

    scaled = -(rates_ref[...].T * rate_scale)
    v_in.wait()
    for h in range(16):
        cols = pl.ds(h * 256, 256)
        gsrc[:, cols] = (scaled[:, h : h + 1] * vbuf[:, cols].astype(F32)).astype(BF16)
    gbuf[pl.ds(0, 128), :] = gsrc[:, pl.ds(mine, 256)]
    send(1, gsrc, gbuf, range(1, 5))
    for slot in range(5, 16):
        send(0, k_ref, kbuf, (slot,))
        send(1, gsrc, gbuf, (slot,))
    grad[...] = jnp.zeros_like(grad)

    for m in range(3):
        @pl.when(c == owner)
        def _():
            weights_in(m).wait()

        @pl.when(c != owner)
        def _():
            weights_over(m).wait_recv()

        wb[m] = wf[m].astype(BF16)

    def grad_block(start, size):
        toks = pl.ds(pl.multiple_of(start, 256), size)
        keys, gout = kbuf[toks, :], gbuf[toks, :]
        pre = dot_nt(wb[0], keys)
        gate = dot_nt(wb[1], keys)
        back = dot_nt(wb[2], gout)
        sg = 0.5 + 0.5 * jnp.tanh(0.5 * pre)
        silu = pre * sg
        hidden = (silu * gate).astype(BF16)
        grad_gate = (back * silu).astype(BF16)
        grad_pre = ((back * gate) * (sg + silu - silu * sg)).astype(BF16)
        grad[0] += dot_nn(grad_pre, keys)
        grad[1] += dot_nn(grad_gate, keys)
        grad[2] += dot_nn(hidden, gout)

    def slot_wait(kind, target, slot):
        remote(
            target.at[pl.ds(0, 128)], target.at[pl.ds(slot * 128, 128)],
            a2a_send.at[kind, slot], a2a_recv.at[kind, slot], dev(1),
        ).wait_recv()

    k_own.wait()

    def block(t, carry):
        @pl.when(t > 0)
        def _():
            slot_wait(0, kbuf, 2 * t)
            slot_wait(1, gbuf, 2 * t)

        slot_wait(0, kbuf, 2 * t + 1)
        slot_wait(1, gbuf, 2 * t + 1)
        grad_block(t * 256, 256)
        return carry

    lax.fori_loop(0, 6, block, 0)
    for slot in range(12, 16):
        slot_wait(0, kbuf, slot)
        slot_wait(1, gbuf, slot)
    send(2, q_ref, qbuf, Q_ORDER)
    q_own.start()
    wo_rows = pl.ds(pl.multiple_of(c * 512, 512), 512)
    wo_in = pltpu.make_async_copy(wout_ref, wout.at[wo_rows], loc_sem.at[4])
    wo_over = remote(wout_ref, wout.at[wo_rows], wo_send, wo_recv, dev(dc=1))

    core_copies, z_copies = [], []

    def last_piece(n, dz):
        kept = pl.ds(pl.multiple_of(c * 512 + ((z + dz) % 4) * 128, 128), 128)
        given = pl.ds(pl.multiple_of((1 - c) * 512 + ((z + dz) % 4) * 128, 128), 128)
        keys, gout = kbuf[pl.ds(1536, 512), :], gbuf[pl.ds(1536, 512), :]

        def both(m):
            return jnp.concatenate([wb[m, given, :], wb[m, kept, :]], axis=0)

        pre = dot_nt(both(0), keys)
        gate = dot_nt(both(1), keys)
        back = dot_nt(both(2), gout)
        sg = 0.5 + 0.5 * jnp.tanh(0.5 * pre)
        silu = pre * sg
        hidden = (silu * gate).astype(BF16)
        grad_gate = (back * silu).astype(BF16)
        grad_pre = ((back * gate) * (sg + silu - silu * sg)).astype(BF16)
        for m, sums in ((0, dot_nn(grad_pre, keys)), (1, dot_nn(grad_gate, keys)), (2, dot_nn(hidden, gout))):
            csend[n, m] = (grad[m, given, :] + sums[:128]).astype(BF16)
            grad[m, kept, :] += sums[128:]
        copy = remote(csend.at[n], crecv.at[n], cs_sem.at[n], cr_sem.at[n], dev(dc=1))
        copy.start()
        core_copies.append(copy)

    def piece(n, dz, part):
        rows = pl.ds(pl.multiple_of(c * 512 + ((z + dz) % 4) * 128 + part * 64, 64), 64)
        return grad[:, rows, :] + crecv[n, :, pl.ds(part * 64, 64), :].astype(F32)

    def z_send(n, value, dz):
        zsend[n] = value.astype(BF16)
        copy = remote(zsend.at[n], zrecv.at[n], zs_sem.at[n], zr_sem.at[n], dev(dz=dz))
        copy.start()
        z_copies.append(copy)

    last_piece(0, 2)
    last_piece(1, 1)
    core_copies[0].wait_recv()
    z_send(0, piece(0, 2, 0), 1)
    z_send(1, piece(0, 2, 1), -1)
    last_piece(2, 3)
    core_copies[1].wait_recv()
    z_send(2, piece(1, 1, 1), 1)
    last_piece(3, 0)
    core_copies[2].wait_recv()
    z_send(3, piece(2, 3, 0), -1)
    z_copies[0].wait_recv()
    z_send(4, piece(1, 1, 0) + zrecv[0].astype(F32), 1)
    z_copies[1].wait_recv()
    z_send(5, piece(2, 3, 1) + zrecv[1].astype(F32), -1)
    wo_in.start()
    wo_over.start()
    core_copies[3].wait_recv()
    own = pl.ds(row_own, 128)

    @pl.when(c == owner)
    def _():
        mom_in.wait()

    @pl.when(c != owner)
    def _():
        mom_over.wait_recv()

    base = wf[:, own, :] - 0.9 * mom[...] - (grad[:, own, :] + crecv[3].astype(F32))
    grad[:, own, :] = base
    row_old = jnp.sqrt(jnp.sum(jnp.square(wf[0:2, own, :]), axis=2, keepdims=True))
    column_old = jnp.sqrt(jnp.sum(jnp.square(wf[2]), axis=0, keepdims=True))
    for n in range(2, 6):
        z_copies[n].wait_recv()
    others = jnp.concatenate(
        [zrecv[4].astype(F32) + zrecv[3].astype(F32), zrecv[2].astype(F32) + zrecv[5].astype(F32)], axis=1
    )
    updated = grad[:, own, :] - others
    row_new = jnp.sum(jnp.square(updated[0:2]), axis=2, keepdims=True)
    normed[0:2, own, :] = (updated[0:2] * row_old / jnp.sqrt(row_new + 1e-06)).astype(BF16)
    normed[2, own, :] = updated[2].astype(BF16)

    def half_rows(dz, part):
        return pl.ds(pl.multiple_of(c * 512 + ((z + dz) % 4) * 128 + part * 64, 64), 64)

    n_copies, p_copies = [], []

    def n_send(n, rows, dz):
        copy = remote(normed.at[:, rows], normed.at[:, rows], ns_sem.at[n], nr_sem.at[n], dev(dz=dz))
        copy.start()
        n_copies.append(copy)

    def p_send(n, rows):
        copy = remote(normed.at[:, rows], normed.at[:, rows], ps_sem.at[n], pr_sem.at[n], dev(dc=1))
        copy.start()
        p_copies.append(copy)

    n_send(0, half_rows(0, 0), 1)
    n_send(1, half_rows(0, 1), -1)
    n_send(2, half_rows(0, 1), 1)
    n_send(3, half_rows(0, 0), -1)
    p_send(6, own)
    n_copies[0].wait_recv()
    n_send(4, half_rows(-1, 0), 1)
    p_send(0, half_rows(-1, 0))
    n_copies[1].wait_recv()
    n_send(5, half_rows(1, 1), -1)
    p_send(1, half_rows(1, 1))
    for n, dz, part in ((2, -1, 1), (3, 1, 0), (4, 2, 0), (5, 2, 1)):
        n_copies[n].wait_recv()
        p_send(n, half_rows(dz, part))
    for copy in p_copies:
        copy.wait_recv()
    column_new = jnp.sum(jnp.square(normed[2].astype(F32)), axis=0, keepdims=True)
    cscale[...] = column_old / jnp.sqrt(column_new + 1e-06)

    q_own.wait()

    def applied(query):
        hidden = []
        for i in range(4):
            rows = pl.ds(i * 256, 256)
            pre = dot_nt(query, normed[0, rows, :])
            gate = dot_nt(query, normed[1, rows, :])
            hidden.append((pre * (0.5 + 0.5 * jnp.tanh(0.5 * pre)) * gate).astype(BF16))
        return (dot_nn(jnp.concatenate(hidden, axis=1), normed[2]) * cscale[...]).astype(BF16)

    my_cols = pl.ds(pl.multiple_of(y * 256, 256), 256)
    o_copies = []

    def apply_group(first):
        for slot in range(first, first + 4):
            if slot > 0:
                slot_wait(2, qbuf, slot)
        osend[pl.ds(first * 128, 512), :] = applied(qbuf[pl.ds(first * 128, 512), :])
        for slot in range(first, first + 4):
            dx, dy = Q_OFFSETS[slot]
            if dy == 0:
                obuf[pl.ds(dx * 128, 128), my_cols] = osend[pl.ds(slot * 128, 128), :]
            else:
                copy = remote(
                    osend.at[pl.ds(slot * 128, 128)], obuf.at[pl.ds(dx * 128, 128), my_cols],
                    os_sem.at[dx, dy], or_sem.at[dx, dy], dev(dy=-dy),
                )
                copy.start()
                o_copies.append(copy)

    def apply_far(half):
        result = applied(
            jnp.concatenate([qbuf[pl.ds(slot * 128 + half * 64, 64), :] for slot in range(4, 8)], axis=0)
        )
        obuf[pl.ds(256 + half * 64, 64), my_cols] = result[0:64]
        for n in (3, 1, 2):
            rows = pl.ds((4 + n) * 128 + half * 64, 64)
            osend[rows, :] = result[n * 64 : n * 64 + 64]
            dy = Q_OFFSETS[4 + n][1]
            copy = remote(
                osend.at[rows], obuf.at[pl.ds(256 + half * 64, 64), my_cols],
                os_sem.at[2 + 2 * half, dy], or_sem.at[2 + 2 * half, dy], dev(dy=-dy),
            )
            copy.start()
            o_copies.append(copy)

    for slot in range(4, 8):
        slot_wait(2, qbuf, slot)
    apply_far(0)
    apply_far(1)
    apply_group(8)

    wo_in.wait()
    wo_over.wait_recv()

    def o_wait(dx, rows=128):
        for dy in (1, 2, 3):
            remote(
                osend.at[pl.ds(0, rows)], obuf.at[pl.ds(0, rows), pl.ds(0, 256)],
                os_sem.at[dx, dy], or_sem.at[dx, dy], dev(1),
            ).wait_recv()

    def message(kind, j, up):
        return remote(
            msend.at[kind, j], mrecv.at[kind, j], ms_sem.at[kind, j], mr_sem.at[kind, j], dev(1 if up else -1)
        )

    def product(first, rows, j, width=512):
        return dot_nn(obuf[pl.ds(first, rows), :], wout[:, pl.ds(pl.multiple_of(j * width, width), width)])

    def far_message(kind, part):
        return remote(
            fsend.at[kind, part], frecv.at[kind, part], fs_sem.at[kind, part], fr_sem.at[kind, part],
            dev(-1 if kind else 1),
        )

    for half in (0, 1):
        o_wait(2 + 2 * half, 64)

        def far(n, carry):
            j, kind = n // 2, n % 2
            fsend[kind, 2 * half + j] = product(256 + half * 64, 64, j + 2 * kind, 1024).astype(BF16)
            far_message(kind, 2 * half + j).start()
            return carry

        for n in range(4):
            far(n, 0)
    apply_group(12)
    apply_group(0)
    o_wait(1)
    o_wait(3)

    def near(j, carry):
        msend[0, j] = product(384, 128, j + 4).astype(BF16)
        message(0, j, True).start()
        msend[1, j] = product(128, 128, j).astype(BF16)
        message(1, j, False).start()
        return carry

    lax.fori_loop(0, 4, near, 0)

    def relay_part(j, carry):
        stash[0, j] = product(384, 128, j)
        stash[1, j] = product(128, 128, j + 4)
        return carry

    lax.fori_loop(0, 4, relay_part, 0)

    for j in range(4):
        for kind in (0, 1):
            if j % 2 == 0:
                far_message(kind, j // 2).wait_recv()
                far_message(kind, 2 + j // 2).wait_recv()
            for half in (0, 1):
                rows, cols = pl.ds(half * 64, 64), pl.ds((j % 2) * 512, 512)
                msend[2 + kind, j, rows, :] = (
                    stash[kind, j, rows, :] + frecv[kind, 2 * half + j // 2, :, cols].astype(F32)
                ).astype(BF16)
            message(2 + kind, j, kind == 0).start()

    o_wait(0)

    def rest(j, carry):
        total[j] = product(0, 128, j)
        return carry

    lax.fori_loop(0, 8, rest, 0)

    def finish(j, carry):
        low = pl.ds(pl.multiple_of(j * 512, 512), 512)
        high = pl.ds(pl.multiple_of(j * 512 + 2048, 512), 512)
        message(1, j, False).wait_recv()
        message(0, j, True).wait_recv()
        message(2, j, True).wait_recv()
        out_ref[:, low] = (total[j] + mrecv[1, j].astype(F32) + mrecv[2, j].astype(F32)).astype(BF16)
        message(3, j, False).wait_recv()
        out_ref[:, high] = (total[j + 4] + mrecv[0, j].astype(F32) + mrecv[3, j].astype(F32)).astype(BF16)
        return carry

    lax.fori_loop(0, 4, finish, 0)

    for copy in a2a + core_copies + z_copies + n_copies + p_copies + o_copies:
        copy.wait_send()
    wo_over.wait_send()

    @pl.when(c == owner)
    def _():
        for m in range(3):
            weights_over(m).wait_send()
        mom_over.wait_send()

    def drain(j, carry):
        for kind in range(4):
            message(kind, j, kind % 2 == 0).wait_send()
        for kind in range(2):
            far_message(kind, j).wait_send()
        return carry

    lax.fori_loop(0, 4, drain, 0)


def shards(query_rows, key_rows, value_rows, token_rates, fast_weights, momentum, out_weight):
    tokens = key_rows.shape[0] * lax.axis_size("head") * lax.axis_size("ctx")
    anywhere = pl.BlockSpec(memory_space=pl.ANY)
    vmem = pl.BlockSpec(memory_space=pltpu.VMEM)
    dma = pltpu.SemaphoreType.DMA
    return pl.pallas_call(
        functools.partial(kernel, float(tokens) ** (-0.5)),
        out_shape=pltpu.VMEM((128, 4096), BF16),
        in_specs=[anywhere, anywhere, anywhere, vmem, anywhere, anywhere, anywhere],
        out_specs=vmem,
        scratch_shapes=[
            pltpu.VMEM((128, 4096), BF16),
            pltpu.VMEM((128, 4096), BF16),
            pltpu.VMEM((2048, 256), BF16),
            pltpu.VMEM((2048, 256), BF16),
            pltpu.VMEM((2048, 256), BF16),
            pltpu.VMEM((3, 1024, 256), F32),
            pltpu.VMEM((3, 1024, 256), BF16),
            pltpu.VMEM((3, 128, 256), F32),
            pltpu.VMEM((3, 1024, 256), F32),
            pltpu.VMEM((4, 3, 128, 256), BF16),
            pltpu.VMEM((4, 3, 128, 256), BF16),
            pltpu.VMEM((6, 3, 64, 256), BF16),
            pltpu.VMEM((6, 3, 64, 256), BF16),
            pltpu.VMEM((3, 1024, 256), BF16),
            pltpu.VMEM((1, 256), F32),
            pltpu.VMEM((2048, 256), BF16),
            pltpu.VMEM((512, 1024), BF16),
            pltpu.VMEM((1024, 4096), BF16),
            pltpu.VMEM((2, 4, 128, 512), F32),
            pltpu.VMEM((8, 128, 512), F32),
            pltpu.VMEM((4, 4, 128, 512), BF16),
            pltpu.VMEM((4, 4, 128, 512), BF16),
            pltpu.VMEM((2, 4, 64, 1024), BF16),
            pltpu.VMEM((2, 4, 64, 1024), BF16),
            dma((3, 16)), dma((3, 16)), dma((6,)), dma((4,)), dma((4,)), dma((4,)), dma((4,)), dma((6,)), dma((6,)),
            dma((6,)), dma((6,)), dma((7,)), dma((7,)), dma((5, 4)), dma((5, 4)), dma((4, 4)), dma((4, 4)),
            dma((2, 4)), dma((2, 4)), dma(()), dma(()),
        ],
        compiler_params=pltpu.CompilerParams(collective_id=0, has_side_effects=True, vmem_limit_bytes=62 * 2**20),
        name="ttt_layer",
    )(query_rows, key_rows, value_rows, token_rates.T, fast_weights, momentum, out_weight)


def solution(mesh):
    placed = (
        P(("head", "ctx"), None),
        P(("head", "ctx"), None),
        P(("head", "ctx"), None),
        P(("head", "ctx"), None),
        P("head", None, None, None),
        P("head", None, None, None),
        P("head", None),
    )
    return jax.shard_map(
        shards, mesh=mesh, in_specs=placed, out_specs=P(("head", "ctx"), None), check_vma=False
    )
```

```python
import functools

import jax
import jax.numpy as jnp
from jax import lax
from jax.experimental import pallas as pl
from jax.experimental.pallas import tpu as pltpu
from jax.sharding import PartitionSpec as P

MESH = pl.DeviceIdType.MESH
F32 = jnp.float32
BF16 = jnp.bfloat16

K_OFFSETS = (
    (0, 0), (2, 2), (1, 1), (3, 3),
    (2, 1), (1, 2), (2, 3), (3, 2),
    (2, 0), (0, 2), (1, 3), (3, 1),
    (1, 0), (0, 1), (3, 0), (0, 3),
)
Q_OFFSETS = (
    (0, 0), (0, 1), (0, 3), (0, 2),
    (2, 0), (2, 1), (2, 3), (2, 2),
    (1, 2), (3, 2), (1, 1), (3, 3),
    (1, 3), (3, 1), (1, 0), (3, 0),
)
Q_ORDER = (7, 10, 11, 5, 8, 6, 9, 4, 3, 12, 13, 14, 1, 15, 2)


NT = (((1,), (1,)), ((), ()))


def dot_nt(a, b):
    return lax.dot_general(a, b, NT, preferred_element_type=F32)


def dot_nn(a, b):
    return jnp.dot(a, b, preferred_element_type=F32)


def kernel(
    rate_scale,
    q_ref, k_ref, v_ref, rates_ref, fast_ref, mom_ref, wout_ref,
    out_ref,
    vbuf, gsrc, kbuf, gbuf, qbuf, wf, wb, mom, grad,
    csend, crecv, zsend, zrecv, normed, cscale,
    osend, obuf, wout, stash, total, msend, mrecv, fsend, frecv,
    a2a_send, a2a_recv, loc_sem, w_send, w_recv, cs_sem, cr_sem, zs_sem, zr_sem,
    ns_sem, nr_sem, ps_sem, pr_sem, os_sem, or_sem, ms_sem, mr_sem, fs_sem, fr_sem, wo_send, wo_recv,
):
    head, ctx = lax.axis_index("head"), lax.axis_index("ctx")
    x, c = head // 2, head % 2
    z, y = ctx // 4, ctx % 4
    owner = y // 2
    local = y % 2

    def dev(dx=0, dy=0, dz=0, dc=0):
        return (((x + dx) % 4) * 2 + (c + dc) % 2, ((z + dz) % 4) * 4 + (y + dy) % 4)

    def remote(src, dst, ssem, rsem, where):
        return pltpu.make_async_remote_copy(
            src_ref=src, dst_ref=dst, send_sem=ssem, recv_sem=rsem, device_id=where, device_id_type=MESH
        )

    barrier = pltpu.get_barrier_semaphore()
    for dx, dy in K_OFFSETS[1:]:
        pl.semaphore_signal(barrier, inc=1, device_id=dev(dx, dy), device_id_type=MESH)
    for dz in (1, 2, 3):
        pl.semaphore_signal(barrier, inc=1, device_id=dev(dz=dz), device_id_type=MESH)
    pl.semaphore_signal(barrier, inc=1, device_id=dev(dc=1), device_id_type=MESH)

    v_in = pltpu.make_async_copy(v_ref, vbuf, loc_sem.at[5])
    v_in.start()
    mine = pl.multiple_of((x * 4 + y) * 256, 256)
    k_own = pltpu.make_async_copy(k_ref.at[:, pl.ds(mine, 256)], kbuf.at[pl.ds(0, 128)], a2a_recv.at[0, 0])
    q_own = pltpu.make_async_copy(q_ref.at[:, pl.ds(mine, 256)], qbuf.at[pl.ds(0, 128)], a2a_recv.at[2, 0])
    k_own.start()

    pl.semaphore_wait(barrier, 19)

    def block_copy(kind, source, target, slot):
        dx, dy = (Q_OFFSETS if kind == 2 else K_OFFSETS)[slot]
        to = pl.multiple_of((((x + dx) % 4) * 4 + (y + dy) % 4) * 256, 256)
        return remote(
            source.at[:, pl.ds(to, 256)], target.at[pl.ds(slot * 128, 128)],
            a2a_send.at[kind, slot], a2a_recv.at[kind, slot], dev(dx, dy),
        )

    def weights_in(m):
        return pltpu.make_async_copy(fast_ref.at[local, m], wf.at[m], loc_sem.at[m])

    def weights_over(m):
        return remote(fast_ref.at[local, m], wf.at[m], w_send.at[m], w_recv.at[m], dev(dc=1))

    row_own = pl.multiple_of(c * 512 + z * 128, 128)
    row_other = pl.multiple_of((1 - c) * 512 + z * 128, 128)
    mom_in = pltpu.make_async_copy(mom_ref.at[local, :, pl.ds(row_own, 128)], mom, loc_sem.at[3])
    mom_over = remote(mom_ref.at[local, :, pl.ds(row_other, 128)], mom, w_send.at[3], w_recv.at[3], dev(dc=1))

    a2a = []

    def send(kind, source, target, slots):
        for slot in slots:
            copy = block_copy(kind, source, target, slot)
            copy.start()
            a2a.append(copy)

    send(0, k_ref, kbuf, range(1, 5))

    @pl.when(c == owner)
    def _():
        for m in range(3):
            weights_in(m).start()
        mom_in.start()
        for m in range(3):
            weights_over(m).start()
        mom_over.start()

    scaled = -(rates_ref[...].T * rate_scale)
    v_in.wait()
    for h in range(16):
        cols = pl.ds(h * 256, 256)
        gsrc[:, cols] = (scaled[:, h : h + 1] * vbuf[:, cols].astype(F32)).astype(BF16)
    gbuf[pl.ds(0, 128), :] = gsrc[:, pl.ds(mine, 256)]
    send(1, gsrc, gbuf, range(1, 5))
    for slot in range(5, 16):
        send(0, k_ref, kbuf, (slot,))
        send(1, gsrc, gbuf, (slot,))
    grad[...] = jnp.zeros_like(grad)

    for m in range(3):
        @pl.when(c == owner)
        def _():
            weights_in(m).wait()

        @pl.when(c != owner)
        def _():
            weights_over(m).wait_recv()

        wb[m] = wf[m].astype(BF16)

    def grad_block(start, size):
        toks = pl.ds(pl.multiple_of(start, 256), size)
        keys, gout = kbuf[toks, :], gbuf[toks, :]
        pre = dot_nt(wb[0], keys)
        gate = dot_nt(wb[1], keys)
        back = dot_nt(wb[2], gout)
        sg = 0.5 + 0.5 * jnp.tanh(0.5 * pre)
        silu = pre * sg
        hidden = (silu * gate).astype(BF16)
        grad_gate = (back * silu).astype(BF16)
        grad_pre = ((back * gate) * (sg + silu - silu * sg)).astype(BF16)
        grad[0] += dot_nn(grad_pre, keys)
        grad[1] += dot_nn(grad_gate, keys)
        grad[2] += dot_nn(hidden, gout)

    def slot_wait(kind, target, slot):
        remote(
            target.at[pl.ds(0, 128)], target.at[pl.ds(slot * 128, 128)],
            a2a_send.at[kind, slot], a2a_recv.at[kind, slot], dev(1),
        ).wait_recv()

    k_own.wait()

    def block(t, carry):
        @pl.when(t > 0)
        def _():
            slot_wait(0, kbuf, 2 * t)
            slot_wait(1, gbuf, 2 * t)

        slot_wait(0, kbuf, 2 * t + 1)
        slot_wait(1, gbuf, 2 * t + 1)
        grad_block(t * 256, 256)
        return carry

    lax.fori_loop(0, 6, block, 0)
    for slot in range(12, 16):
        slot_wait(0, kbuf, slot)
        slot_wait(1, gbuf, slot)
    send(2, q_ref, qbuf, Q_ORDER)
    q_own.start()
    wo_rows = pl.ds(pl.multiple_of(c * 512, 512), 512)
    wo_in = pltpu.make_async_copy(wout_ref, wout.at[wo_rows], loc_sem.at[4])
    wo_over = remote(wout_ref, wout.at[wo_rows], wo_send, wo_recv, dev(dc=1))

    core_copies, z_copies = [], []

    def last_piece(n, dz):
        kept = pl.ds(pl.multiple_of(c * 512 + ((z + dz) % 4) * 128, 128), 128)
        given = pl.ds(pl.multiple_of((1 - c) * 512 + ((z + dz) % 4) * 128, 128), 128)
        keys, gout = kbuf[pl.ds(1536, 512), :], gbuf[pl.ds(1536, 512), :]

        def both(m):
            return jnp.concatenate([wb[m, given, :], wb[m, kept, :]], axis=0)

        pre = dot_nt(both(0), keys)
        gate = dot_nt(both(1), keys)
        back = dot_nt(both(2), gout)
        sg = 0.5 + 0.5 * jnp.tanh(0.5 * pre)
        silu = pre * sg
        hidden = (silu * gate).astype(BF16)
        grad_gate = (back * silu).astype(BF16)
        grad_pre = ((back * gate) * (sg + silu - silu * sg)).astype(BF16)
        for m, sums in ((0, dot_nn(grad_pre, keys)), (1, dot_nn(grad_gate, keys)), (2, dot_nn(hidden, gout))):
            csend[n, m] = (grad[m, given, :] + sums[:128]).astype(BF16)
            grad[m, kept, :] += sums[128:]
        copy = remote(csend.at[n], crecv.at[n], cs_sem.at[n], cr_sem.at[n], dev(dc=1))
        copy.start()
        core_copies.append(copy)

    order = (2, 0, 1)

    def piece(n, dz, part, m):
        rows = pl.ds(pl.multiple_of(c * 512 + ((z + dz) % 4) * 128 + part * 64, 64), 64)
        return grad[m, rows, :] + crecv[n, m, pl.ds(part * 64, 64), :].astype(F32)

    def z_copy(n, m, dz):
        return remote(zsend.at[n, m], zrecv.at[n, m], zs_sem.at[n, m], zr_sem.at[n, m], dev(dz=dz))

    def z_send(n, m, value, dz):
        zsend[n, m] = value.astype(BF16)
        copy = z_copy(n, m, dz)
        copy.start()
        z_copies.append(copy)

    last_piece(0, 2)
    last_piece(1, 1)
    core_copies[0].wait_recv()
    for m in order:
        z_send(0, m, piece(0, 2, 0, m), 1)
        z_send(1, m, piece(0, 2, 1, m), -1)
    last_piece(2, 3)
    core_copies[1].wait_recv()
    for m in order:
        z_send(2, m, piece(1, 1, 1, m), 1)
    last_piece(3, 0)
    core_copies[2].wait_recv()
    for m in order:
        z_send(3, m, piece(2, 3, 0, m), -1)
    for m in order:
        z_copy(0, m, 1).wait_recv()
        z_send(4, m, piece(1, 1, 0, m) + zrecv[0, m].astype(F32), 1)
        z_copy(1, m, -1).wait_recv()
        z_send(5, m, piece(2, 3, 1, m) + zrecv[1, m].astype(F32), -1)
    wo_in.start()
    wo_over.start()
    core_copies[3].wait_recv()
    own = pl.ds(row_own, 128)

    @pl.when(c == owner)
    def _():
        mom_in.wait()

    @pl.when(c != owner)
    def _():
        mom_over.wait_recv()

    base = wf[:, own, :] - 0.9 * mom[...] - (grad[:, own, :] + crecv[3].astype(F32))
    grad[:, own, :] = base
    row_old = jnp.sqrt(jnp.sum(jnp.square(wf[0:2, own, :]), axis=2, keepdims=True))
    column_old = jnp.sqrt(jnp.sum(jnp.square(wf[2]), axis=0, keepdims=True))
    def half_rows(dz, part):
        return pl.ds(pl.multiple_of(c * 512 + ((z + dz) % 4) * 128 + part * 64, 64), 64)

    n_copies, p_copies = {}, []

    def n_send(n, m, rows, dz):
        n_copies[n, m] = remote(normed.at[m, rows], normed.at[m, rows], ns_sem.at[n, m], nr_sem.at[n, m], dev(dz=dz))
        n_copies[n, m].start()

    def p_send(n, m, rows):
        copy = remote(normed.at[m, rows], normed.at[m, rows], ps_sem.at[n, m], pr_sem.at[n, m], dev(dc=1))
        copy.start()
        p_copies.append(copy)

    for m in order:
        for n in range(2, 6):
            z_copy(n, m, 1).wait_recv()
        others = jnp.concatenate(
            [zrecv[4, m].astype(F32) + zrecv[3, m].astype(F32), zrecv[2, m].astype(F32) + zrecv[5, m].astype(F32)], axis=0
        )
        updated = grad[m, own, :] - others
        if m < 2:
            row_new = jnp.sum(jnp.square(updated), axis=1, keepdims=True)
            updated = updated * row_old[m] / jnp.sqrt(row_new + 1e-06)
        normed[m, own, :] = updated.astype(BF16)
        n_send(0, m, half_rows(0, 0), 1)
        n_send(1, m, half_rows(0, 1), -1)
        n_send(2, m, half_rows(0, 1), 1)
        n_send(3, m, half_rows(0, 0), -1)
        p_send(6, m, own)
    for m in order:
        n_copies[0, m].wait_recv()
        n_send(4, m, half_rows(-1, 0), 1)
        p_send(0, m, half_rows(-1, 0))
        n_copies[1, m].wait_recv()
        n_send(5, m, half_rows(1, 1), -1)
        p_send(1, m, half_rows(1, 1))
    for pair in (((2, -1, 1), (3, 1, 0)), ((4, 2, 0), (5, 2, 1))):
        for m in order:
            for n, dz, part in pair:
                n_copies[n, m].wait_recv()
                p_send(n, m, half_rows(dz, part))
    for copy in p_copies:
        copy.wait_recv()
    column_new = jnp.sum(jnp.square(normed[2].astype(F32)), axis=0, keepdims=True)
    cscale[...] = column_old / jnp.sqrt(column_new + 1e-06)

    q_own.wait()

    def applied(query):
        hidden = []
        for i in range(4):
            rows = pl.ds(i * 256, 256)
            pre = dot_nt(query, normed[0, rows, :])
            gate = dot_nt(query, normed[1, rows, :])
            hidden.append((pre * (0.5 + 0.5 * jnp.tanh(0.5 * pre)) * gate).astype(BF16))
        return (dot_nn(jnp.concatenate(hidden, axis=1), normed[2]) * cscale[...]).astype(BF16)

    my_cols = pl.ds(pl.multiple_of(y * 256, 256), 256)
    o_copies = []

    def apply_group(first):
        for slot in range(first, first + 4):
            if slot > 0:
                slot_wait(2, qbuf, slot)
        osend[pl.ds(first * 128, 512), :] = applied(qbuf[pl.ds(first * 128, 512), :])
        for slot in range(first, first + 4):
            dx, dy = Q_OFFSETS[slot]
            if dy == 0:
                obuf[pl.ds(dx * 128, 128), my_cols] = osend[pl.ds(slot * 128, 128), :]
            else:
                copy = remote(
                    osend.at[pl.ds(slot * 128, 128)], obuf.at[pl.ds(dx * 128, 128), my_cols],
                    os_sem.at[dx, dy], or_sem.at[dx, dy], dev(dy=-dy),
                )
                copy.start()
                o_copies.append(copy)

    def apply_far(half):
        result = applied(
            jnp.concatenate([qbuf[pl.ds(slot * 128 + half * 64, 64), :] for slot in range(4, 8)], axis=0)
        )
        obuf[pl.ds(256 + half * 64, 64), my_cols] = result[0:64]
        for n in (3, 1, 2):
            rows = pl.ds((4 + n) * 128 + half * 64, 64)
            osend[rows, :] = result[n * 64 : n * 64 + 64]
            dy = Q_OFFSETS[4 + n][1]
            copy = remote(
                osend.at[rows], obuf.at[pl.ds(256 + half * 64, 64), my_cols],
                os_sem.at[2 + 2 * half, dy], or_sem.at[2 + 2 * half, dy], dev(dy=-dy),
            )
            copy.start()
            o_copies.append(copy)

    for slot in range(4, 8):
        slot_wait(2, qbuf, slot)
    apply_far(0)
    apply_far(1)
    apply_group(8)
    apply_group(12)

    wo_in.wait()
    wo_over.wait_recv()

    def o_wait(dx, rows=128):
        for dy in (1, 2, 3):
            remote(
                osend.at[pl.ds(0, rows)], obuf.at[pl.ds(0, rows), pl.ds(0, 256)],
                os_sem.at[dx, dy], or_sem.at[dx, dy], dev(1),
            ).wait_recv()

    def message(kind, j, up):
        return remote(
            msend.at[kind, j], mrecv.at[kind, j], ms_sem.at[kind, j], mr_sem.at[kind, j], dev(1 if up else -1)
        )

    def product(first, rows, j):
        return dot_nn(obuf[pl.ds(first, rows), :], wout[:, pl.ds(pl.multiple_of(j * 512, 512), 512)])

    def far_message(kind, part):
        return remote(
            fsend.at[kind, part], frecv.at[kind, part], fs_sem.at[kind, part], fr_sem.at[kind, part],
            dev(-1 if kind else 1),
        )

    for half in (0, 1):
        o_wait(2 + 2 * half, 64)

        def far(j, carry):
            for kind in (0, 1):
                fsend[kind, 4 * half + j] = product(256 + half * 64, 64, j + 4 * kind).astype(BF16)
                far_message(kind, 4 * half + j).start()
            return carry

        lax.fori_loop(0, 4, far, 0)
    o_wait(1)
    o_wait(3)

    def near(j, carry):
        msend[0, j] = product(384, 128, j + 4).astype(BF16)
        message(0, j, True).start()
        msend[1, j] = product(128, 128, j).astype(BF16)
        message(1, j, False).start()
        return carry

    lax.fori_loop(0, 4, near, 0)

    apply_group(0)
    def relay_part(j, carry):
        stash[0, j] = product(384, 128, j)
        stash[1, j] = product(128, 128, j + 4)
        return carry

    lax.fori_loop(0, 4, relay_part, 0)

    for j in range(4):
        for kind in (0, 1):
            for half in (0, 1):
                far_message(kind, 4 * half + j).wait_recv()
                rows = pl.ds(half * 64, 64)
                msend[2 + kind, j, rows, :] = (
                    stash[kind, j, rows, :] + frecv[kind, 4 * half + j].astype(F32)
                ).astype(BF16)
            message(2 + kind, j, kind == 0).start()

    o_wait(0)

    def rest(j, carry):
        total[j] = product(0, 128, j)
        return carry

    lax.fori_loop(0, 8, rest, 0)

    def finish(j, carry):
        low = pl.ds(pl.multiple_of(j * 512, 512), 512)
        high = pl.ds(pl.multiple_of(j * 512 + 2048, 512), 512)
        message(1, j, False).wait_recv()
        message(0, j, True).wait_recv()
        message(2, j, True).wait_recv()
        out_ref[:, low] = (total[j] + mrecv[1, j].astype(F32) + mrecv[2, j].astype(F32)).astype(BF16)
        message(3, j, False).wait_recv()
        out_ref[:, high] = (total[j + 4] + mrecv[0, j].astype(F32) + mrecv[3, j].astype(F32)).astype(BF16)
        return carry

    lax.fori_loop(0, 4, finish, 0)

    for copy in a2a + core_copies + z_copies + list(n_copies.values()) + p_copies + o_copies:
        copy.wait_send()
    wo_over.wait_send()

    @pl.when(c == owner)
    def _():
        for m in range(3):
            weights_over(m).wait_send()
        mom_over.wait_send()

    def drain(j, carry):
        for kind in range(4):
            message(kind, j, kind % 2 == 0).wait_send()
        for kind in range(2):
            far_message(kind, j).wait_send()
            far_message(kind, 4 + j).wait_send()
        return carry

    lax.fori_loop(0, 4, drain, 0)


def shards(query_rows, key_rows, value_rows, token_rates, fast_weights, momentum, out_weight):
    tokens = key_rows.shape[0] * lax.axis_size("head") * lax.axis_size("ctx")
    anywhere = pl.BlockSpec(memory_space=pl.ANY)
    vmem = pl.BlockSpec(memory_space=pltpu.VMEM)
    dma = pltpu.SemaphoreType.DMA
    return pl.pallas_call(
        functools.partial(kernel, float(tokens) ** (-0.5)),
        out_shape=pltpu.VMEM((128, 4096), BF16),
        in_specs=[anywhere, anywhere, anywhere, vmem, anywhere, anywhere, anywhere],
        out_specs=vmem,
        scratch_shapes=[
            pltpu.VMEM((128, 4096), BF16),
            pltpu.VMEM((128, 4096), BF16),
            pltpu.VMEM((2048, 256), BF16),
            pltpu.VMEM((2048, 256), BF16),
            pltpu.VMEM((2048, 256), BF16),
            pltpu.VMEM((3, 1024, 256), F32),
            pltpu.VMEM((3, 1024, 256), BF16),
            pltpu.VMEM((3, 128, 256), F32),
            pltpu.VMEM((3, 1024, 256), F32),
            pltpu.VMEM((4, 3, 128, 256), BF16),
            pltpu.VMEM((4, 3, 128, 256), BF16),
            pltpu.VMEM((6, 3, 64, 256), BF16),
            pltpu.VMEM((6, 3, 64, 256), BF16),
            pltpu.VMEM((3, 1024, 256), BF16),
            pltpu.VMEM((1, 256), F32),
            pltpu.VMEM((2048, 256), BF16),
            pltpu.VMEM((512, 1024), BF16),
            pltpu.VMEM((1024, 4096), BF16),
            pltpu.VMEM((2, 4, 128, 512), F32),
            pltpu.VMEM((8, 128, 512), F32),
            pltpu.VMEM((4, 4, 128, 512), BF16),
            pltpu.VMEM((4, 4, 128, 512), BF16),
            pltpu.VMEM((2, 8, 64, 512), BF16),
            pltpu.VMEM((2, 8, 64, 512), BF16),
            dma((3, 16)), dma((3, 16)), dma((6,)), dma((4,)), dma((4,)), dma((4,)), dma((4,)), dma((6, 3)), dma((6, 3)),
            dma((6, 3)), dma((6, 3)), dma((7, 3)), dma((7, 3)), dma((5, 4)), dma((5, 4)), dma((4, 4)), dma((4, 4)),
            dma((2, 8)), dma((2, 8)), dma(()), dma(()),
        ],
        compiler_params=pltpu.CompilerParams(collective_id=0, has_side_effects=True, vmem_limit_bytes=62 * 2**20),
        name="ttt_layer",
    )(query_rows, key_rows, value_rows, token_rates.T, fast_weights, momentum, out_weight)


def solution(mesh):
    placed = (
        P(("head", "ctx"), None),
        P(("head", "ctx"), None),
        P(("head", "ctx"), None),
        P(("head", "ctx"), None),
        P("head", None, None, None),
        P("head", None, None, None),
        P("head", None),
    )
    return jax.shard_map(
        shards, mesh=mesh, in_specs=placed, out_specs=P(("head", "ctx"), None), check_vma=False
    )
```
